32 devices in a mesh: dp: 4 (over z), seq: 8 (over y, x, core).
Axes of the slice: x: 2, y: 2, z: 4, core: 2. Of those that a mesh axis runs over, the one named last changes fastest.
Arguments:
- tokens: bfloat16 [4, 4096, 768], P('dp', 'seq'), may hold values from -6 to 6
- cotangent: bfloat16 [4, 4096, 768], P('dp', 'seq'), may hold values from -6 to 6
- norm_gain: bfloat16 [768], P(('dp', 'seq')), may hold values from 0.5 to 1.5
- in_weight: bfloat16 [768, 3352], P(('dp', 'seq')), may hold values from -2 to 2
- conv_weight: bfloat16 [4, 1792], P(None, ('dp', 'seq')), may hold values from -3 to 3
- conv_bias: bfloat16 [1792], P(('dp', 'seq')), may hold values from -3 to 3
- dt_bias: float32 [24], replicated, may hold values from -8 to -6
- a_log: float32 [24], replicated, may hold values from -10 to 0
- d_skip: float32 [24], replicated, may hold values from 0.5 to 2
- gate_gain: bfloat16 [1536], P(('dp', 'seq')), may hold values from 0.5 to 1.5
- out_weight: bfloat16 [1536, 768], P(('dp', 'seq')), may hold values from -0.15625 to 0.15625
Outputs:
- block_out: bfloat16 [4, 4096, 768], P('dp', 'seq')
- input_grad: bfloat16 [4, 4096, 768], P('dp', 'seq')
- norm_grad: float32 [768], P(('dp', 'seq'))
- inward_grad: float32 [768, 3352], P(('dp', 'seq'))
- kernel_grad: float32 [4, 1792], P(None, ('dp', 'seq'))
- offset_grad: float32 [1792], P(('dp', 'seq'))
- step_grad: float32 [24], replicated
- decay_grad: float32 [24], replicated
- skip_grad: float32 [24], replicated
- gain_grad: float32 [1536], P(('dp', 'seq'))
- outward_grad: float32 [1536, 768], P(('dp', 'seq'))
The draws below stay inside these ranges and needn't reach their ends.
All inputs are finite; a program needn't handle non-finite values.
Results may differ from the reference program's by a relative error of at most 0.018.
Values may be sent and summed in bfloat16 or wider, within the bound.
A program may use at most 256 MiB of HBM per device.

```python
import math
import jax
import jax.numpy as jnp
from jax import lax

D = 768
NHEADS = 24
HEADDIM = 64
NSTATE = 128
KCONV = 4
GROUP = 256
DI = 1536
DC = 1792
NP = 3352
LENGTH = 4096
BATCH = 4


def draw_in_weight(key, part):
    values = jnp.clip(jax.random.normal(key, (D, NP), jnp.float32), -4.0, 4.0) / math.sqrt(D)
    columns = jnp.arange(NP)
    factor = jnp.where(columns >= 2 * DI + 2 * NSTATE, 4.0, 1.0)
    return (values * factor[None, :]).astype(jnp.bfloat16)


def draw_a_log(key, part):
    key_one, key_two = jax.random.split(jax.random.fold_in(key, 17))
    spread = jax.random.uniform(key_one, (NHEADS,), jnp.float32)
    choose = jax.random.uniform(key_two, (NHEADS,), jnp.float32)
    portion = 0.5
    lasting = math.log(0.3 / (LENGTH * 0.05)) + spread * math.log(1.0 / 0.3)
    fading = math.log(0.3) + spread * math.log(1.0 / 0.3)
    return jnp.where(choose < portion, lasting, fading).astype(jnp.float32)


def raised(result, own_key, source, target, parts, factor):
    owner, partner = [(jnp.arange(result.shape[dim]) // (result.shape[dim] // parts)).reshape([-1 if axis == dim else 1 for axis in range(result.ndim)]) for dim in (source, target)]
    chosen = jax.random.permutation(own_key, parts)[partner]
    strong = (owner == chosen) | (owner == (partner + parts // 2) % parts)
    return jnp.where(strong, factor * result, result)


def steps_of(own_key, extent, cuts, low, top_value):
    def one(axis_at, blocks):
        heights = jax.random.uniform(jax.random.fold_in(jax.random.fold_in(own_key, 6), axis_at), (blocks,), jnp.float32, low / len(cuts), top_value / len(cuts))
        return jnp.repeat(jnp.exp(heights), extent[axis_at] // blocks).reshape((-1,) + (1,) * (len(extent) - axis_at - 1))

    loudness = one(*cuts[0])
    for cut in cuts[1:]:
        loudness = loudness * one(*cut)
    return loudness


def scatter_about(key, shape, width, reach, cuts=(), kind=jnp.bfloat16):
    drawn = width * jax.random.normal(key, shape, jnp.float32)
    if cuts:
        drawn = drawn * steps_of(key, shape, cuts, -0.22, 0.18)
    return jnp.clip(drawn, -reach, reach).astype(kind)


def gaussian_with(key, extent, scale, reach, cuts, heavy, held_as=jnp.bfloat16):
    result = scale * jax.random.normal(key, extent, jnp.float32)
    if cuts:
        result = result * steps_of(key, extent, cuts, -0.22, 0.18)
    return jnp.clip(raised(result, jax.random.fold_in(key, 3), *heavy), -reach, reach).astype(held_as)


def setup_inputs(seed: int = 0) -> dict:
    key_of = jax.random.split(jax.random.key(seed), 12)
    return {
        "tokens": gaussian_with(key_of[0], (BATCH, LENGTH, D), 1.0, 6.0, ((0, 4), (1, 8)), (1, 2, 8, 2.0)),
        "cotangent": scatter_about(key_of[1], (BATCH, LENGTH, D), 1.0, 6.0, ((0, 4), (1, 8))),
        "norm_gain": jnp.clip(1.0 + 0.1 * jax.random.normal(key_of[2], (D,), jnp.float32), 0.5, 1.5).astype(jnp.bfloat16),
        "in_weight": draw_in_weight(jax.random.fold_in(key_of[11], 71), 0),
        "conv_weight": scatter_about(key_of[4], (KCONV, DC), KCONV ** -0.5, 3.0, ((1, 32),)),
        "conv_bias": scatter_about(key_of[5], (DC,), 0.5, 3.0, ((0, 32),)),
        "dt_bias": jnp.clip(jax.random.uniform(key_of[6], (NHEADS,), jnp.float32, -8.0, -6.0), -8.0, -6.0),
        "a_log": draw_a_log(jax.random.fold_in(key_of[11], 71), 0),
        "d_skip": jnp.clip(jax.random.uniform(key_of[8], (NHEADS,), jnp.float32, 0.5, 2.0), 0.5, 2.0),
        "gate_gain": jnp.clip(1.0 + 0.1 * jax.random.normal(key_of[9], (DI,), jnp.float32), 0.5, 1.5).astype(jnp.bfloat16),
        "out_weight": scatter_about(key_of[10], (DI, D), DI ** -0.5, 0.15625, ((0, 32),)),
    }


epsilon = 1e-05
highest = lax.Precision.HIGHEST

@jax.custom_vjp
def low(v):
    return lax.optimization_barrier(v.astype(jnp.bfloat16)).astype(jnp.float32)

@jax.custom_vjp
def low_back(v):
    return v

def low_keep(v):
    return (low(v), None)

def low_pass(kept, grad):
    return (grad,)

def back_keep(v):
    return (v, None)

def back_low(kept, grad):
    return (low(grad),)
low.defvjp(low_keep, low_pass)
low_back.defvjp(back_keep, back_low)

def rms_scale(values, weight):
    return values * lax.rsqrt(lax.optimization_barrier(jnp.mean(values * values, axis=-1, keepdims=True)) + epsilon) * weight

def group_step(hidden_state, pieces):
    heads_in, input_map, output_map, step_size, log_decay = pieces
    running = jnp.cumsum(log_decay, axis=0)
    block_len = running.shape[0]
    causal = (jnp.arange(block_len)[:, None] >= jnp.arange(block_len)[None, :])[:, :, None]
    spread = jnp.where(causal, running[:, None, :] - running[None, :, :], 0.0)
    decays = jnp.where(causal, jnp.exp(spread), 0.0)
    scores = jnp.dot(output_map, input_map.T, precision=highest)
    weights = scores[:, :, None] * decays * step_size[None, :, :]
    output = jnp.einsum('tsh,shp->thp', weights, heads_in, precision=highest)
    output = output + jnp.exp(running)[:, :, None] * jnp.einsum('tn,hpn->thp', output_map, hidden_state, precision=highest)
    to_end = jnp.exp(running[-1][None, :] - running) * step_size
    added_in = jnp.einsum('shp,sn->hpn', heads_in * to_end[:, :, None], input_map, precision=highest)
    hidden_state = jnp.exp(running[-1])[:, None, None] * hidden_state + added_in
    return (hidden_state, output)

def ssd_sequence(heads_in, input_map, output_map, step_size, log_decay):
    blocks = LENGTH // GROUP
    pieces = (heads_in.reshape(blocks, GROUP, NHEADS, HEADDIM), input_map.reshape(blocks, GROUP, NSTATE), output_map.reshape(blocks, GROUP, NSTATE), step_size.reshape(blocks, GROUP, NHEADS), log_decay.reshape(blocks, GROUP, NHEADS))
    initial = jnp.zeros((NHEADS, HEADDIM, NSTATE), heads_in.dtype)
    final_state, outputs = lax.scan(jax.checkpoint(group_step), initial, pieces)
    return outputs.reshape(LENGTH, NHEADS, HEADDIM)

def block_forward(inputs, norm_gain, in_matrix, conv_taps, conv_offset, step_bias, log_rate, skip_gain, gate_gain, out_matrix):
    normed = low(rms_scale(inputs, norm_gain))
    projected = low_back(low(jnp.dot(normed, in_matrix, precision=highest)))
    gate_z = projected[:, :DI]
    conv_in = projected[:, DI:DI + DC]
    step_raw = projected[:, DI + DC:]
    padded = jnp.concatenate([jnp.zeros((KCONV - 1, DC), inputs.dtype), conv_in], axis=0)
    pre_act = conv_offset + sum((conv_taps[position] * padded[position:position + LENGTH] for position in range(KCONV)))
    activated = jax.nn.silu(pre_act)
    heads_in = activated[:, :DI].reshape(LENGTH, NHEADS, HEADDIM)
    input_map = activated[:, DI:DI + NSTATE]
    output_map = activated[:, DI + NSTATE:]
    step_size = jax.nn.softplus(step_raw + step_bias)
    log_decay = -step_size * jnp.exp(log_rate)
    summed = ssd_sequence(heads_in, input_map, output_map, step_size, log_decay)
    with_skip = (summed + skip_gain[:, None] * heads_in).reshape(LENGTH, DI)
    gated_in = with_skip * jax.nn.silu(gate_z)
    gate_low = low(rms_scale(gated_in, gate_gain))
    return inputs + jnp.dot(gate_low, out_matrix, precision=highest)

def add_trees(first_tree, second_tree):
    return jax.tree.map(jnp.add, first_tree, second_tree)

def reference(tokens, cotangent, norm_gain, in_weight, conv_weight, conv_bias, dt_bias, a_log, d_skip, gate_gain, out_weight):
    params = (norm_gain.astype(jnp.float32), in_weight.astype(jnp.float32), conv_weight.astype(jnp.float32), conv_bias.astype(jnp.float32), dt_bias.astype(jnp.float32), a_log.astype(jnp.float32), d_skip.astype(jnp.float32), gate_gain.astype(jnp.float32), out_weight.astype(jnp.float32))

    def one_sequence(totals, pieces):
        seq_in, seq_grad = pieces
        output, pullback = jax.vjp(block_forward, seq_in.astype(jnp.float32), *params)
        grads = pullback(seq_grad.astype(jnp.float32))
        totals = add_trees(totals, tuple(grads[1:]))
        return (totals, (output.astype(jnp.bfloat16), grads[0].astype(jnp.bfloat16)))
    zeros = tuple((jnp.zeros_like(param) for param in params))
    totals, (outputs, in_grads) = lax.scan(one_sequence, zeros, (tokens, cotangent))
    return (outputs, in_grads, totals[0], totals[1], totals[2], totals[3], totals[4], totals[5], totals[6], totals[7], totals[8])
```

```python
import functools

import jax
import jax.numpy as jnp
from jax import lax
from jax.experimental import pallas as pl
from jax.experimental.pallas import tpu as pltpu
from jax.sharding import PartitionSpec as P

MESH = pl.DeviceIdType.MESH
NHEADS = 24
HEADDIM = 64
NSTATE = 128
KCONV = 4
DI = 1536
DC = 1792
Q = 128
LANES = 128
PAIRS = DI // LANES
HALF = DI // 2
epsilon = 1e-05
highest = lax.Precision.HIGHEST
f32 = jnp.float32
bf16 = jnp.bfloat16


def mm(a, b):
    return lax.dot_general(a, b, (((1,), (0,)), ((), ())), preferred_element_type=f32)


def mm_nt(a, b):
    return lax.dot_general(a, b, (((1,), (1,)), ((), ())), preferred_element_type=f32)


def mm_exact(a, b):
    return lax.dot_general(
        a, b, (((1,), (0,)), ((), ())), precision=highest, preferred_element_type=f32
    )


def sigmoid(v):
    return 1.0 / (1.0 + jnp.exp(-v))


def fold_rows(v):
    return jnp.sum(v.reshape(v.shape[0] // 8, 8, v.shape[1]), axis=0)


def ssd_kernel(
    seq_size,
    proj,
    grad_low,
    taps,
    cbias,
    heads,
    gain,
    gate_low,
    grad_proj,
    sum_conv,
    sum_gate,
    sum_head,
    cpad,
    act,
    dsilu,
    gpad,
    yint,
    yst,
    ws,
    sg,
    gs,
    ex_e,
    ex_f,
    ex_dt,
    cum,
    cum_t,
    dts,
    logd,
    sgm,
    grad_a,
    states,
    adjs,
    s0,
    g0,
    conv_edge,
    grad_edge,
    full_send,
    full_recv,
    half_send,
    half_recv,
    swap_send,
    swap_recv,
    log_send,
    log_recv,
    edge_sems,
    full_sems,
    half_sems,
    swap_sems,
    log_sems,
    swap_hold,
    passed,
):
    length = proj.shape[0]
    chunks = length // Q
    me = lax.axis_index("seq")
    bits = seq_size.bit_length() - 1
    bit = [(me // (1 << r)) % 2 for r in range(bits)]
    partner = [me + (1 - 2 * bit[r]) * (1 << r) for r in range(bits)]
    side = bit[0]

    barrier = pltpu.get_barrier_semaphore()
    for other in partner:
        pl.semaphore_signal(barrier, inc=1, device_id={"seq": other}, device_id_type=MESH)

    @pl.when(me > 0)
    def _():
        pl.semaphore_signal(barrier, inc=1, device_id={"seq": me - 1}, device_id_type=MESH)

    @pl.when(me < seq_size - 1)
    def _():
        pl.semaphore_signal(barrier, inc=1, device_id={"seq": me + 1}, device_id_type=MESH)

    pl.semaphore_wait(barrier, bits + jnp.where(me > 0, 1, 0) + jnp.where(me < seq_size - 1, 1, 0))

    def edge_copy():
        return pltpu.make_async_remote_copy(
            src_ref=proj.at[pl.ds(length - 16, 16), pl.ds(DI, DC)],
            dst_ref=conv_edge,
            send_sem=edge_sems.at[0],
            recv_sem=edge_sems.at[1],
            device_id={"seq": me + 1},
            device_id_type=MESH,
        )

    def grad_edge_copy():
        return pltpu.make_async_remote_copy(
            src_ref=gpad.at[pl.ds(0, 8), :],
            dst_ref=grad_edge,
            send_sem=edge_sems.at[2],
            recv_sem=edge_sems.at[3],
            device_id={"seq": me - 1},
            device_id_type=MESH,
        )

    def exchange(src, dst, sems, index, other):
        return pltpu.make_async_remote_copy(
            src_ref=src,
            dst_ref=dst,
            send_sem=sems.at[index, 0],
            recv_sem=sems.at[index, 1],
            device_id={"seq": other},
            device_id_type=MESH,
        )

    @pl.when(me < seq_size - 1)
    def _():
        edge_copy().start()

    lane_head = lax.broadcasted_iota(jnp.int32, (NHEADS, DI), 1) // HEADDIM
    spread_m = (lane_head == lax.broadcasted_iota(jnp.int32, (NHEADS, DI), 0)).astype(bf16)
    rows_i = lax.broadcasted_iota(jnp.int32, (Q, Q), 0)
    cols_i = lax.broadcasted_iota(jnp.int32, (Q, Q), 1)
    lower = (rows_i >= cols_i)
    lower_f = lower.astype(f32)
    upper_f = (rows_i <= cols_i).astype(f32)
    strict_upper = rows_i < cols_i
    low_lane = lax.broadcasted_iota(jnp.int32, (Q, LANES), 1) < HEADDIM

    def gather_m(p):
        lane = lax.broadcasted_iota(jnp.int32, (LANES, NHEADS), 0) // HEADDIM + 2 * p
        return (lane == lax.broadcasted_iota(jnp.int32, (LANES, NHEADS), 1)).astype(bf16)

    def pair(p):
        return pl.ds(p * LANES, LANES)

    def blockdiag(v):
        zero = jnp.zeros_like(v)
        return jnp.concatenate([jnp.where(low_lane, v, zero), jnp.where(low_lane, zero, v)], axis=0)

    def spread_row(row):
        hi = row.astype(bf16)
        rest = row - hi.astype(f32)
        mid = rest.astype(bf16)
        lo = (rest - mid.astype(f32)).astype(bf16)
        return mm(hi, spread_m) + mm(mid, spread_m) + mm(lo, spread_m)

    dt_bias = heads[0:1, :]
    rate = jnp.exp(heads[1:2, :])
    skip_wide = spread_row(jnp.broadcast_to(heads[2:3, :], (8, NHEADS)))[0:1, :]

    def rates(c, carry):
        rows = pl.ds(pl.multiple_of(c * Q, Q), Q)
        raw = proj[rows, pl.ds(DI + DC, NHEADS)].astype(f32) + dt_bias
        dt = jnp.maximum(raw, 0.0) + jnp.log1p(jnp.exp(-jnp.abs(raw)))
        ld = -dt * rate
        run = mm_exact(lower_f, ld)
        dts[rows, :] = dt
        logd[rows, :] = ld
        sgm[rows, :] = sigmoid(raw)
        cum[rows, :] = run
        wide = jnp.concatenate([run, jnp.zeros((Q, LANES - NHEADS), f32)], axis=1)
        cum_t[c] = wide.T[0:NHEADS, :]
        last = run[Q - 1 : Q, :]
        ex_e[rows, :] = mm(jnp.exp(run).astype(bf16), spread_m).astype(bf16)
        ex_f[rows, :] = mm(jnp.exp(last - run).astype(bf16), spread_m).astype(bf16)
        ex_dt[rows, :] = mm(dt.astype(bf16), spread_m).astype(bf16)
        return carry + last

    log_total = lax.fori_loop(0, chunks, rates, jnp.zeros((1, NHEADS), f32))

    def load_conv(c, carry):
        rows = pl.ds(pl.multiple_of(c * Q, Q), Q)
        cpad[pl.ds(pl.multiple_of(c * Q + 8, 8), Q), :] = proj[rows, pl.ds(DI, DC)].astype(f32)
        return carry

    lax.fori_loop(0, chunks, load_conv, 0)

    @pl.when(me > 0)
    def _():
        edge_copy().wait_recv()
        cpad[0:8, :] = conv_edge[...].astype(f32)[8:16, :]

    @pl.when(me == 0)
    def _():
        cpad[0:8, :] = jnp.zeros((8, DC), f32)

    @pl.when(me < seq_size - 1)
    def _():
        edge_copy().wait_send()

    def conv_block(c, block):
        lanes = pl.ds(block * LANES, LANES)
        window = cpad[pl.ds(pl.multiple_of(c * Q, Q), Q + 8), lanes]
        pre = cbias[0:1, lanes] + sum(
            taps[k : k + 1, lanes] * window[5 + k : 5 + k + Q, :] for k in range(KCONV)
        )
        gate = sigmoid(pre)
        value = pre * gate
        rows = pl.ds(pl.multiple_of(c * Q, Q), Q)
        act[rows, lanes] = value
        dsilu[rows, lanes] = gate + value * (1.0 - gate)

    def local_states(c, carry):
        rows = pl.ds(pl.multiple_of(c * Q, Q), Q)
        for block in range(DC // LANES):
            conv_block(c, block)
        decay = spread_row(jnp.exp(jnp.broadcast_to(cum_t[c][:, Q - 1 : Q], (NHEADS, 8)).T))[0:1, :]
        in_t = act[rows, pl.ds(DI, NSTATE)].T.astype(bf16)
        for p in range(PAIRS):
            xw = act[rows, pair(p)] * (ex_f[rows, pair(p)].astype(f32) * ex_dt[rows, pair(p)].astype(f32))
            states[c + 1, :, pair(p)] = decay[:, p * LANES : (p + 1) * LANES] * states[
                c, :, pair(p)
            ] + mm(in_t, xw.astype(bf16))
        return carry

    states[0] = jnp.zeros((NSTATE, DI), f32)
    lax.fori_loop(0, chunks, local_states, 0)

    log_send[0] = jnp.concatenate(
        [jnp.broadcast_to(log_total, (8, NHEADS)), jnp.zeros((8, LANES - NHEADS), f32)], axis=1
    )


    side_f = side.astype(f32)
    half_lane = (lax.broadcasted_iota(jnp.int32, (NHEADS, HALF), 1) + side * HALF) // HEADDIM
    spread_half = (half_lane == lax.broadcasted_iota(jnp.int32, (NHEADS, HALF), 0)).astype(bf16)

    def widen(row, matrix):
        hi = row.astype(bf16)
        rest = row - hi.astype(f32)
        mid = rest.astype(bf16)
        return (mm(hi, matrix) + mm(mid, matrix))[0:1, :]

    def scan_ops(way, total, out):
        near = [(bit[r] if way == 0 else 1 - bit[r]).astype(f32) for r in range(bits)]

        def full():
            return exchange(full_send.at[way], full_recv.at[way], full_sems, way, partner[0])

        def half(r):
            k = way * bits + r
            return exchange(half_send.at[k], half_recv.at[k], half_sems, k, partner[r])

        def swap():
            return exchange(swap_send.at[way], swap_recv.at[way], swap_sems, way, partner[0])

        def logs(r):
            return exchange(log_send.at[r], log_recv.at[r], log_sems, r, partner[r])

        def start():
            for s in range(2):
                full_send[way, s] = total[:, s * HALF : (s + 1) * HALF].astype(bf16)
            full().start()
            if way == 0:
                logs(0).start()
            passed[way] = jnp.zeros((8, NHEADS), f32)

        def step(r):
            if r == 0:
                full().wait()
            else:
                half(r).wait()
            if way == 0:
                logs(r).wait()
                if r + 1 < bits:
                    log_send[r + 1] = log_send[r] + log_recv[r]
            log_mine = log_send[r][:, 0:NHEADS]
            log_theirs = log_recv[r][:, 0:NHEADS]
            if r == 0:
                mine = full_send[way, side].astype(f32)
                theirs = full_recv[way, side].astype(f32)
                held = jnp.zeros((NSTATE, HALF), f32)
            else:
                mine = half_send[way * bits + r].astype(f32)
                theirs = half_recv[way * bits + r].astype(f32)
                factor = near[r] * widen(jnp.exp(passed[way]), spread_half)
                held = swap_hold[way] + factor * theirs
                passed[way] = passed[way] + near[r] * log_theirs
            if r + 1 < bits:
                keep = widen(jnp.exp((1.0 - near[r]) * log_theirs), spread_half)
                take = widen(jnp.exp(near[r] * log_mine), spread_half)
                half_send[way * bits + r + 1] = (keep * mine + take * theirs).astype(bf16)
                half(r + 1).start()
                if way == 0:
                    logs(r + 1).start()
                swap_hold[way] = held
            else:
                swap_send[way] = held.astype(bf16)
                swap().start()

        def finish():
            swap().wait()
            decay = widen(jnp.exp(near[0] * log_recv[0][:, 0:NHEADS]), spread_m)
            for s in range(2):
                own = side_f if s == 1 else 1.0 - side_f
                part = own * swap_send[way].astype(f32) + (1.0 - own) * swap_recv[way].astype(f32)
                out[:, s * HALF : (s + 1) * HALF] = (
                    near[0] * full_recv[way, s].astype(f32)
                    + decay[:, s * HALF : (s + 1) * HALF] * part
                )

        def after(c):
            for r in range(min(bits, chunks)):
                pl.when(c == r)(functools.partial(step, r))

        def rest():
            for r in range(min(bits, chunks), bits):
                step(r)
            finish()

        return start, after, rest

    start, after, rest = scan_ops(0, states.at[chunks], s0)
    start()

    def rows_of(c):
        return pl.ds(pl.multiple_of(c * Q, Q), Q)

    def intra_forward(c, carry):
        rows = rows_of(c)
        in_low = act[rows, pl.ds(DI, NSTATE)].astype(bf16)
        out_low = act[rows, pl.ds(DI + NSTATE, NSTATE)].astype(bf16)
        scores = mm_nt(out_low, in_low) * lower_f
        for p in range(PAIRS):
            parts = []
            for h in (2 * p, 2 * p + 1):
                spread = cum[rows, h : h + 1] - cum_t[c, h : h + 1, :]
                parts.append((scores * jnp.exp(jnp.minimum(spread, 0.0))).astype(bf16))
            stepped = (act[rows, pair(p)] * ex_dt[rows, pair(p)].astype(f32)).astype(bf16)
            yst[rows, pair(p)] = mm(jnp.concatenate(parts, axis=1), blockdiag(stepped))
        after(c)
        return carry

    lax.fori_loop(0, chunks, intra_forward, 0)
    rest()

    sum_conv[...] = jnp.zeros_like(sum_conv)
    sum_gate[...] = jnp.zeros_like(sum_gate)
    gain_wide = gain[0:1, :]

    def state_decay(c):
        last = jnp.broadcast_to(cum_t[c][:, Q - 1 : Q], (NHEADS, 8))
        wide = jnp.concatenate([last, jnp.zeros((LANES - NHEADS, 8), f32)], axis=0)
        return wide.T[:, 0:NHEADS]

    def gating(c, before):
        rows = rows_of(c)
        decay_before = widen(jnp.exp(before), spread_m)
        out_now = act[rows, pl.ds(DI + NSTATE, NSTATE)]
        out_low = out_now.astype(bf16)
        out_t = out_now.T.astype(bf16)
        squares = jnp.zeros((Q, LANES), f32)
        for p in range(PAIRS):
            state = states[c, :, pair(p)] + decay_before[:, p * LANES : (p + 1) * LANES] * s0[
                :, pair(p)
            ]
            states[c, :, pair(p)] = state
            reached = ex_e[rows, pair(p)].astype(f32) * mm(out_low, state.astype(bf16))
            with_skip = (
                yst[rows, pair(p)]
                + reached
                + skip_wide[:, p * LANES : (p + 1) * LANES] * act[rows, pair(p)]
            )
            z = proj[rows, pair(p)].astype(f32)
            sig = sigmoid(z)
            gated = with_skip * (z * sig)
            squares += gated * gated
            yint[:, pair(p)] = reached
            ws[:, pair(p)] = with_skip
            sg[:, pair(p)] = sig
        norm = lax.rsqrt(jnp.sum(squares, axis=1, keepdims=True) * (1.0 / DI) + epsilon)
        inner = jnp.zeros((Q, LANES), f32)
        for p in range(PAIRS):
            z = proj[rows, pair(p)].astype(f32)
            gated = ws[:, pair(p)] * (z * sg[:, pair(p)])
            gain_p = gain_wide[:, p * LANES : (p + 1) * LANES]
            gate_low[rows, pair(p)] = (gated * norm * gain_p).astype(bf16)
            inner += grad_low[rows, pair(p)] * gain_p * gated
            sum_gate[0:8, pair(p)] += fold_rows(grad_low[rows, pair(p)] * (gated * norm))
        mean = jnp.sum(inner, axis=1, keepdims=True) * (1.0 / DI)
        pull = norm * norm * norm * mean
        later = jnp.zeros((Q, NHEADS), f32)
        for p in range(PAIRS):
            z = proj[rows, pair(p)].astype(f32)
            sig = sg[:, pair(p)]
            with_skip = ws[:, pair(p)]
            gain_p = gain_wide[:, p * LANES : (p + 1) * LANES]
            gated = with_skip * (z * sig)
            grad_gated = norm * (grad_low[rows, pair(p)] * gain_p) - gated * pull
            grad = grad_gated * (z * sig)
            gs[rows, pair(p)] = grad
            grad_z = grad_gated * with_skip * (sig * (1.0 + z * (1.0 - sig)))
            grad_proj[rows, pair(p)] = grad_z.astype(bf16)
            sum_gate[8:16, pair(p)] += fold_rows(grad * act[rows, pair(p)])
            later += mm((grad * yint[:, pair(p)]).astype(bf16), gather_m(p))
            scaled = (grad * ex_e[rows, pair(p)].astype(f32)).astype(bf16)
            adjs[c, :, pair(p)] = mm(out_t, scaled)
        grad_a[rows, :] = mm_exact(upper_f, later)
        return before + state_decay(c)

    lax.fori_loop(0, chunks, gating, jnp.zeros((8, NHEADS), f32))

    adjs[chunks] = jnp.zeros((NSTATE, DI), f32)

    def local_adjoints(i, carry):
        c = chunks - 1 - i
        decay = widen(jnp.exp(state_decay(c)), spread_m)
        for p in range(PAIRS):
            adjs[c, :, pair(p)] = (
                decay[:, p * LANES : (p + 1) * LANES] * adjs[c + 1, :, pair(p)]
                + adjs[c, :, pair(p)]
            )
        return carry

    lax.fori_loop(0, chunks, local_adjoints, 0)
    start, after, rest = scan_ops(1, adjs.at[0], g0)
    start()

    def intra_backward(c, carry):
        rows = rows_of(c)
        in_low = act[rows, pl.ds(DI, NSTATE)].astype(bf16)
        out_low = act[rows, pl.ds(DI + NSTATE, NSTATE)].astype(bf16)
        scores = mm_nt(in_low, out_low) * upper_f
        grad_scores = jnp.zeros((Q, Q), f32)
        tails = upper_f.T.astype(bf16)
        found = []
        for p in range(PAIRS):
            grad = gs[rows, pair(p)].astype(bf16)
            stepped = (act[rows, pair(p)] * ex_dt[rows, pair(p)].astype(f32)).astype(bf16)
            values = mm_nt(blockdiag(stepped), grad)
            weights, crosses = [], []
            for i, h in enumerate((2 * p, 2 * p + 1)):
                spread = cum_t[c, h : h + 1, :] - cum[rows, h : h + 1]
                decays = jnp.exp(jnp.minimum(spread, 0.0))
                weights.append((scores * decays).astype(bf16))
                part = decays * values[i * Q : (i + 1) * Q, :]
                grad_scores += part
                crosses.append((part * scores).astype(bf16))
            yst[rows, pair(p)] = mm(jnp.concatenate(weights, axis=1), blockdiag(grad))
            sums = mm(jnp.concatenate(crosses, axis=0), tails)
            for i in range(2):
                picked = jnp.where(strict_upper, sums[i * Q : (i + 1) * Q, :], 0.0)
                found.append(jnp.sum(picked, axis=0, keepdims=True))
        found.append(jnp.zeros((LANES - NHEADS, Q), f32))
        grad_a[rows, :] += jnp.concatenate(found, axis=0).T[:, 0:NHEADS]
        grad_low_scores = (grad_scores * upper_f).astype(bf16)
        gpad[rows, pl.ds(DI, NSTATE)] = mm(grad_low_scores, out_low)
        gpad[rows, pl.ds(DI + NSTATE, NSTATE)] = mm((grad_scores * upper_f).T.astype(bf16), in_low)
        after(c)
        return carry

    lax.fori_loop(0, chunks, intra_backward, 0)
    rest()

    sum_head[...] = jnp.zeros_like(sum_head)

    def finish_backward(c, before):
        after_log = jnp.broadcast_to(log_total, (8, NHEADS)) - before - state_decay(c)
        decay_after = widen(jnp.exp(after_log), spread_m)
        rows = rows_of(c)
        in_low = act[rows, pl.ds(DI, NSTATE)].astype(bf16)
        grad_in = gpad[rows, pl.ds(DI, NSTATE)]
        grad_out = gpad[rows, pl.ds(DI + NSTATE, NSTATE)]
        kept = jnp.zeros((Q, NHEADS), f32)
        grad_step = jnp.zeros((Q, NHEADS), f32)
        crossing = jnp.zeros((8, NHEADS), f32)
        for p in range(PAIRS):
            adj = adjs[c + 1, :, pair(p)] + decay_after[:, p * LANES : (p + 1) * LANES] * g0[
                :, pair(p)
            ]
            adj_low = adj.astype(bf16)
            state = states[c, :, pair(p)]
            x = act[rows, pair(p)]
            dt = ex_dt[rows, pair(p)].astype(f32)
            to_end = ex_f[rows, pair(p)].astype(f32)
            grad = gs[rows, pair(p)]
            later = to_end * mm(in_low, adj_low)
            total = yst[rows, pair(p)] + later
            stepped = x * dt
            pick = gather_m(p)
            kept += mm((stepped * later).astype(bf16), pick)
            grad_step += mm((x * total).astype(bf16), pick)
            crossing += mm(fold_rows(adj * state).astype(bf16), pick)
            grad_in += mm_nt((stepped * to_end).astype(bf16), adj_low)
            scaled = (grad * ex_e[rows, pair(p)].astype(f32)).astype(bf16)
            grad_out += mm_nt(scaled, state.astype(bf16))
            grad_x = dt * total + skip_wide[:, p * LANES : (p + 1) * LANES] * grad
            gpad[rows, pair(p)] = grad_x * dsilu[rows, pair(p)]
        gpad[rows, pl.ds(DI, NSTATE)] = grad_in * dsilu[rows, pl.ds(DI, NSTATE)]
        gpad[rows, pl.ds(DI + NSTATE, NSTATE)] = grad_out * dsilu[rows, pl.ds(DI + NSTATE, NSTATE)]
        whole = jnp.exp(state_decay(c))[0:1, :] * jnp.sum(crossing, axis=0, keepdims=True)
        grad_decay = grad_a[rows, :] + mm_exact(lower_f - upper_f * lower_f, kept) + whole
        grad_raw = (grad_step - rate * grad_decay) * sgm[rows, :]
        grad_proj[rows, pl.ds(DI + DC, NHEADS)] = grad_raw.astype(bf16)
        sum_head[0:8, 0:NHEADS] += fold_rows(grad_raw)
        sum_head[8:16, 0:NHEADS] += fold_rows(grad_decay * logd[rows, :])

        @pl.when(jnp.logical_and(c == 0, me > 0))
        def _():
            grad_edge_copy().start()

        return before + state_decay(c)

    lax.fori_loop(0, chunks, finish_backward, jnp.zeros((8, NHEADS), f32))

    @pl.when(me > 0)
    def _():
        grad_edge_copy().wait_send()

    @pl.when(me < seq_size - 1)
    def _():
        grad_edge_copy().wait_recv()
        gpad[pl.ds(length, 8), :] = grad_edge[...]

    @pl.when(me == seq_size - 1)
    def _():
        gpad[pl.ds(length, 8), :] = jnp.zeros((8, DC), f32)

    def conv_backward(c, carry):
        rows = rows_of(c)
        longer = pl.ds(pl.multiple_of(c * Q, Q), Q + 8)
        for block in range(DC // LANES):
            lanes = pl.ds(block * LANES, LANES)
            grads = gpad[longer, lanes]
            inputs = cpad[longer, lanes]
            grad = grads[0:Q, :]
            grad_conv = sum(
                taps[k : k + 1, lanes] * grads[KCONV - 1 - k : KCONV - 1 - k + Q, :]
                for k in range(KCONV)
            )
            grad_proj[rows, pl.ds(DI + block * LANES, LANES)] = grad_conv.astype(bf16)
            for k in range(KCONV):
                sum_conv[8 * k : 8 * k + 8, lanes] += fold_rows(grad * inputs[5 + k : 5 + k + Q, :])
            sum_conv[8 * KCONV : 8 * KCONV + 8, lanes] += fold_rows(grad)
        return carry

    lax.fori_loop(0, chunks, conv_backward, 0)


def ssd_call(seq_size, proj, grad_low, taps, cbias, heads, gain):
    length = proj.shape[0]
    chunks = length // Q
    bits = seq_size.bit_length() - 1
    vmem = lambda shape, kind=f32: pltpu.VMEM(shape, kind)
    space = pl.BlockSpec(memory_space=pltpu.VMEM)
    return pl.pallas_call(
        functools.partial(ssd_kernel, seq_size),
        name="ssd",
        out_shape=(
            jax.ShapeDtypeStruct((length, DI), bf16),
            jax.ShapeDtypeStruct((length, proj.shape[1]), bf16),
            jax.ShapeDtypeStruct((8 * (KCONV + 1), DC), f32),
            jax.ShapeDtypeStruct((16, DI), f32),
            jax.ShapeDtypeStruct((16, LANES), f32),
        ),
        in_specs=[space] * 6,
        out_specs=[space] * 5,
        scratch_shapes=[
            vmem((length + 8, DC)),
            vmem((length, DC)),
            vmem((length, DC)),
            vmem((length + 8, DC)),
            vmem((Q, DI)),
            vmem((length, DI)),
            vmem((Q, DI)),
            vmem((Q, DI)),
            vmem((length, DI)),
            vmem((length, DI), bf16),
            vmem((length, DI), bf16),
            vmem((length, DI), bf16),
            vmem((length, NHEADS)),
            vmem((chunks, NHEADS, Q)),
            vmem((length, NHEADS)),
            vmem((length, NHEADS)),
            vmem((length, NHEADS)),
            vmem((length, NHEADS)),
            vmem((chunks + 1, NSTATE, DI)),
            vmem((chunks + 1, NSTATE, DI)),
            vmem((NSTATE, DI)),
            vmem((NSTATE, DI)),
            vmem((16, DC), bf16),
            vmem((8, DC)),
            vmem((2, 2, NSTATE, HALF), bf16),
            vmem((2, 2, NSTATE, HALF), bf16),
            vmem((2 * bits, NSTATE, HALF), bf16),
            vmem((2 * bits, NSTATE, HALF), bf16),
            vmem((2, NSTATE, HALF), bf16),
            vmem((2, NSTATE, HALF), bf16),
            vmem((bits, 8, LANES)),
            vmem((bits, 8, LANES)),
            pltpu.SemaphoreType.DMA((4,)),
            pltpu.SemaphoreType.DMA((2, 2)),
            pltpu.SemaphoreType.DMA((2 * bits, 2)),
            pltpu.SemaphoreType.DMA((2, 2)),
            pltpu.SemaphoreType.DMA((bits, 2)),
            vmem((2, NSTATE, HALF)),
            vmem((2, 8, NHEADS)),
        ],
        compiler_params=pltpu.CompilerParams(
            collective_id=1, has_side_effects=True, vmem_limit_bytes=62 * 1024 * 1024
        ),
    )(proj, grad_low, taps, cbias, heads, gain)


def rms_scale(values, weight):
    return values * lax.rsqrt(jnp.mean(values * values, axis=-1, keepdims=True) + epsilon) * weight


def local(
    seq_size,
    tokens,
    cotangent,
    norm_gain,
    in_weight,
    conv_weight,
    conv_bias,
    dt_bias,
    a_log,
    d_skip,
    gate_gain,
    out_weight,
):
    axes = ("dp", "seq")
    sizes = [norm_gain.shape[0], conv_weight.size, conv_bias.shape[0], gate_gain.shape[0]]
    packed = jnp.concatenate([norm_gain, conv_weight.reshape(-1), conv_bias, gate_gain])
    packed = lax.all_gather(packed[None].astype(f32), axes, axis=0, tiled=True)
    offsets = [0]
    for size in sizes:
        offsets.append(offsets[-1] + size)
    norm_full = packed[:, : offsets[1]].reshape(-1)
    taps_full = packed[:, offsets[1] : offsets[2]].reshape(-1, KCONV, conv_weight.shape[1])
    taps_full = jnp.swapaxes(taps_full, 0, 1).reshape(KCONV, DC)
    cbias_full = packed[:, offsets[2] : offsets[3]].reshape(1, DC)
    gain_full = packed[:, offsets[3] :].reshape(1, DI)
    in_full = lax.all_gather(in_weight, axes, axis=0, tiled=True)
    out_full = lax.all_gather(out_weight, axes, axis=0, tiled=True)
    heads = jnp.stack([dt_bias, a_log, d_skip])

    tokens = tokens[0]
    cotangent = cotangent[0]
    inputs = tokens.astype(f32)
    normed, norm_back = jax.vjp(rms_scale, inputs, norm_full)
    normed_low = normed.astype(bf16)
    proj = mm(normed_low, in_full).astype(bf16)
    grad_low = mm_nt(cotangent, out_full)
    gate_low, grad_proj, sum_conv, sum_gate, sum_head = ssd_call(
        seq_size, proj, grad_low, taps_full, cbias_full, heads, gain_full
    )
    block_out = (inputs + mm(gate_low, out_full)).astype(bf16)
    outward = lax.dot_general(
        gate_low, cotangent, (((0,), (0,)), ((), ())), preferred_element_type=f32
    )
    inward = lax.dot_general(
        normed_low, grad_proj, (((0,), (0,)), ((), ())), preferred_element_type=f32
    )
    grad_normed = mm_nt(grad_proj, in_full)
    grad_inputs, norm_local = norm_back(grad_normed)
    input_grad = (grad_inputs + cotangent.astype(f32)).astype(bf16)

    conv_local = jnp.sum(sum_conv.reshape(KCONV + 1, 8, DC), axis=1)
    gate_local = jnp.sum(sum_gate.reshape(2, 8, DI), axis=1)
    head_local = jnp.sum(sum_head.reshape(2, 8, LANES), axis=1)[:, :NHEADS]
    skip_local = jnp.sum(gate_local[1].reshape(NHEADS, HEADDIM), axis=1)
    inward = lax.psum_scatter(inward.astype(bf16), axes, scatter_dimension=0, tiled=True)
    outward = lax.psum_scatter(outward.astype(bf16), axes, scatter_dimension=0, tiled=True)
    small = lax.psum(
        jnp.concatenate(
            [norm_local, conv_local.reshape(-1), gate_local[0], head_local.reshape(-1), skip_local]
        ),
        axes,
    )
    rank = lax.axis_index("dp") * seq_size + lax.axis_index("seq")
    at = 0

    def take(count):
        nonlocal at
        at += count
        return small[at - count : at]

    def mine(values, like):
        return lax.dynamic_slice_in_dim(values, rank * like, like, values.ndim - 1)

    norm_grad = mine(take(norm_full.shape[0]), norm_gain.shape[0])
    kernel_grad = mine(take(KCONV * DC).reshape(KCONV, DC), conv_weight.shape[1])
    offset_grad = mine(take(DC), conv_bias.shape[0])
    gain_grad = mine(take(DI), gate_gain.shape[0])
    step_grad, decay_grad, skip_grad = take(NHEADS), take(NHEADS), take(NHEADS)
    return (
        block_out[None],
        input_grad[None],
        norm_grad,
        inward.astype(f32),
        kernel_grad,
        offset_grad,
        step_grad,
        decay_grad,
        skip_grad,
        gain_grad,
        outward.astype(f32),
    )


def solution(mesh):
    both = ("dp", "seq")
    return jax.shard_map(
        functools.partial(local, mesh.shape["seq"]),
        mesh=mesh,
        in_specs=(
            P("dp", "seq", None),
            P("dp", "seq", None),
            P(both),
            P(both, None),
            P(None, both),
            P(both),
            P(),
            P(),
            P(),
            P(both),
            P(both, None),
        ),
        out_specs=(
            P("dp", "seq", None),
            P("dp", "seq", None),
            P(both),
            P(both, None),
            P(None, both),
            P(both),
            P(),
            P(),
            P(),
            P(both),
            P(both, None),
        ),
        check_vma=False,
    )
```

```python
import functools

import jax
import jax.numpy as jnp
from jax import lax
from jax.experimental import pallas as pl
from jax.experimental.pallas import tpu as pltpu
from jax.sharding import PartitionSpec as P

MESH = pl.DeviceIdType.MESH
NHEADS = 24
HEADDIM = 64
NSTATE = 128
KCONV = 4
DI = 1536
DC = 1792
Q = 128
LANES = 128
PAIRS = DI // LANES
HALF = DI // 2
epsilon = 1e-05
highest = lax.Precision.HIGHEST
f32 = jnp.float32
bf16 = jnp.bfloat16


def mm(a, b):
    return lax.dot_general(a, b, (((1,), (0,)), ((), ())), preferred_element_type=f32)


def mm_nt(a, b):
    return lax.dot_general(a, b, (((1,), (1,)), ((), ())), preferred_element_type=f32)


def mm_exact(a, b):
    return lax.dot_general(
        a, b, (((1,), (0,)), ((), ())), precision=highest, preferred_element_type=f32
    )


def sigmoid(v):
    return 1.0 / (1.0 + jnp.exp(-v))


def fold_rows(v):
    return jnp.sum(v.reshape(v.shape[0] // 8, 8, v.shape[1]), axis=0)


def ssd_kernel(
    seq_size,
    proj,
    grad_low,
    taps,
    cbias,
    heads,
    gain,
    gate_low,
    grad_proj,
    sum_conv,
    sum_gate,
    sum_head,
    cpad,
    act,
    dsilu,
    gpad,
    yint,
    yst,
    ws,
    sg,
    gs,
    ex_e,
    ex_f,
    ex_dt,
    cum,
    cum_t,
    dts,
    logd,
    sgm,
    grad_a,
    states,
    adjs,
    s0,
    g0,
    conv_edge,
    grad_edge,
    full_send,
    full_recv,
    half_send,
    half_recv,
    swap_send,
    swap_recv,
    log_send,
    log_recv,
    edge_sems,
    full_sems,
    half_sems,
    swap_sems,
    log_sems,
    swap_hold,
    passed,
):
    length = proj.shape[0]
    chunks = length // Q
    me = lax.axis_index("seq")
    bits = seq_size.bit_length() - 1
    bit = [(me // (1 << r)) % 2 for r in range(bits)]
    partner = [me + (1 - 2 * bit[r]) * (1 << r) for r in range(bits)]
    side = bit[0]

    barrier = pltpu.get_barrier_semaphore()
    for other in partner:
        pl.semaphore_signal(barrier, inc=1, device_id={"seq": other}, device_id_type=MESH)

    @pl.when(me > 0)
    def _():
        pl.semaphore_signal(barrier, inc=1, device_id={"seq": me - 1}, device_id_type=MESH)

    @pl.when(me < seq_size - 1)
    def _():
        pl.semaphore_signal(barrier, inc=1, device_id={"seq": me + 1}, device_id_type=MESH)

    pl.semaphore_wait(barrier, bits + jnp.where(me > 0, 1, 0) + jnp.where(me < seq_size - 1, 1, 0))

    def edge_copy():
        return pltpu.make_async_remote_copy(
            src_ref=proj.at[pl.ds(length - 16, 16), pl.ds(DI, DC)],
            dst_ref=conv_edge,
            send_sem=edge_sems.at[0],
            recv_sem=edge_sems.at[1],
            device_id={"seq": me + 1},
            device_id_type=MESH,
        )

    def grad_edge_copy():
        return pltpu.make_async_remote_copy(
            src_ref=gpad.at[pl.ds(0, 8), :],
            dst_ref=grad_edge,
            send_sem=edge_sems.at[2],
            recv_sem=edge_sems.at[3],
            device_id={"seq": me - 1},
            device_id_type=MESH,
        )

    def exchange(src, dst, sems, index, other):
        return pltpu.make_async_remote_copy(
            src_ref=src,
            dst_ref=dst,
            send_sem=sems.at[index, 0],
            recv_sem=sems.at[index, 1],
            device_id={"seq": other},
            device_id_type=MESH,
        )

    @pl.when(me < seq_size - 1)
    def _():
        edge_copy().start()

    lane_head = lax.broadcasted_iota(jnp.int32, (NHEADS, DI), 1) // HEADDIM
    spread_m = (lane_head == lax.broadcasted_iota(jnp.int32, (NHEADS, DI), 0)).astype(bf16)
    rows_i = lax.broadcasted_iota(jnp.int32, (Q, Q), 0)
    cols_i = lax.broadcasted_iota(jnp.int32, (Q, Q), 1)
    lower = (rows_i >= cols_i)
    lower_f = lower.astype(f32)
    upper_f = (rows_i <= cols_i).astype(f32)
    strict_upper = rows_i < cols_i
    low_lane = lax.broadcasted_iota(jnp.int32, (Q, LANES), 1) < HEADDIM

    def gather_m(p):
        lane = lax.broadcasted_iota(jnp.int32, (LANES, NHEADS), 0) // HEADDIM + 2 * p
        return (lane == lax.broadcasted_iota(jnp.int32, (LANES, NHEADS), 1)).astype(bf16)

    def pair(p):
        return pl.ds(p * LANES, LANES)

    def blockdiag(v):
        zero = jnp.zeros_like(v)
        return jnp.concatenate([jnp.where(low_lane, v, zero), jnp.where(low_lane, zero, v)], axis=0)

    def spread_row(row):
        hi = row.astype(bf16)
        rest = row - hi.astype(f32)
        mid = rest.astype(bf16)
        lo = (rest - mid.astype(f32)).astype(bf16)
        return mm(hi, spread_m) + mm(mid, spread_m) + mm(lo, spread_m)

    dt_bias = heads[0:1, :]
    rate = jnp.exp(heads[1:2, :])
    skip_wide = spread_row(jnp.broadcast_to(heads[2:3, :], (8, NHEADS)))[0:1, :]

    def rates(c, carry):
        rows = pl.ds(pl.multiple_of(c * Q, Q), Q)
        raw = proj[rows, pl.ds(DI + DC, NHEADS)].astype(f32) + dt_bias
        dt = jnp.maximum(raw, 0.0) + jnp.log1p(jnp.exp(-jnp.abs(raw)))
        ld = -dt * rate
        run = mm_exact(lower_f, ld)
        dts[rows, :] = dt
        logd[rows, :] = ld
        sgm[rows, :] = sigmoid(raw)
        cum[rows, :] = run
        wide = jnp.concatenate([run, jnp.zeros((Q, LANES - NHEADS), f32)], axis=1)
        cum_t[c] = wide.T[0:NHEADS, :]
        last = run[Q - 1 : Q, :]
        ex_e[rows, :] = mm(jnp.exp(run).astype(bf16), spread_m).astype(bf16)
        ex_f[rows, :] = mm(jnp.exp(last - run).astype(bf16), spread_m).astype(bf16)
        ex_dt[rows, :] = mm(dt.astype(bf16), spread_m).astype(bf16)
        return carry + last

    log_total = lax.fori_loop(0, chunks, rates, jnp.zeros((1, NHEADS), f32))

    def load_conv(c, carry):
        rows = pl.ds(pl.multiple_of(c * Q, Q), Q)
        cpad[pl.ds(pl.multiple_of(c * Q + 8, 8), Q), :] = proj[rows, pl.ds(DI, DC)].astype(f32)
        return carry

    lax.fori_loop(0, chunks, load_conv, 0)

    @pl.when(me > 0)
    def _():
        edge_copy().wait_recv()
        cpad[0:8, :] = conv_edge[...].astype(f32)[8:16, :]

    @pl.when(me == 0)
    def _():
        cpad[0:8, :] = jnp.zeros((8, DC), f32)

    @pl.when(me < seq_size - 1)
    def _():
        edge_copy().wait_send()

    def conv_block(c, block):
        lanes = pl.ds(block * LANES, LANES)
        window = cpad[pl.ds(pl.multiple_of(c * Q, Q), Q + 8), lanes]
        pre = cbias[0:1, lanes] + sum(
            taps[k : k + 1, lanes] * window[5 + k : 5 + k + Q, :] for k in range(KCONV)
        )
        gate = sigmoid(pre)
        value = pre * gate
        rows = pl.ds(pl.multiple_of(c * Q, Q), Q)
        act[rows, lanes] = value
        dsilu[rows, lanes] = gate + value * (1.0 - gate)

    def local_states(c, carry):
        rows = pl.ds(pl.multiple_of(c * Q, Q), Q)
        for block in range(DC // LANES):
            conv_block(c, block)
        decay = spread_row(jnp.exp(jnp.broadcast_to(cum_t[c][:, Q - 1 : Q], (NHEADS, 8)).T))[0:1, :]
        in_t = act[rows, pl.ds(DI, NSTATE)].T.astype(bf16)
        for p in range(PAIRS):
            xw = act[rows, pair(p)] * (ex_f[rows, pair(p)].astype(f32) * ex_dt[rows, pair(p)].astype(f32))
            states[c + 1, :, pair(p)] = decay[:, p * LANES : (p + 1) * LANES] * states[
                c, :, pair(p)
            ] + mm(in_t, xw.astype(bf16))
        return carry

    states[0] = jnp.zeros((NSTATE, DI), f32)
    lax.fori_loop(0, chunks, local_states, 0)

    log_send[0] = jnp.concatenate(
        [jnp.broadcast_to(log_total, (8, NHEADS)), jnp.zeros((8, LANES - NHEADS), f32)], axis=1
    )


    side_f = side.astype(f32)
    half_lane = (lax.broadcasted_iota(jnp.int32, (NHEADS, HALF), 1) + side * HALF) // HEADDIM
    spread_half = (half_lane == lax.broadcasted_iota(jnp.int32, (NHEADS, HALF), 0)).astype(bf16)

    def widen(row, matrix):
        hi = row.astype(bf16)
        rest = row - hi.astype(f32)
        mid = rest.astype(bf16)
        return (mm(hi, matrix) + mm(mid, matrix))[0:1, :]

    def scan_ops(way, total, out):
        near = [(bit[r] if way == 0 else 1 - bit[r]).astype(f32) for r in range(bits)]

        def full():
            return exchange(full_send.at[way], full_recv.at[way], full_sems, way, partner[0])

        def half(r):
            k = way * bits + r
            return exchange(half_send.at[k], half_recv.at[k], half_sems, k, partner[r])

        def swap():
            return exchange(swap_send.at[way], swap_recv.at[way], swap_sems, way, partner[0])

        def logs(r):
            return exchange(log_send.at[r], log_recv.at[r], log_sems, r, partner[r])

        def start():
            for s in range(2):
                full_send[way, s] = total[:, s * HALF : (s + 1) * HALF].astype(bf16)
            full().start()
            if way == 0:
                logs(0).start()
            passed[way] = jnp.zeros((8, NHEADS), f32)

        def step(r):
            if r == 0:
                full().wait()
            else:
                half(r).wait()
            if way == 0:
                logs(r).wait()
                if r + 1 < bits:
                    log_send[r + 1] = log_send[r] + log_recv[r]
            log_mine = log_send[r][:, 0:NHEADS]
            log_theirs = log_recv[r][:, 0:NHEADS]
            if r == 0:
                mine = full_send[way, side].astype(f32)
                theirs = full_recv[way, side].astype(f32)
                held = jnp.zeros((NSTATE, HALF), f32)
            else:
                mine = half_send[way * bits + r].astype(f32)
                theirs = half_recv[way * bits + r].astype(f32)
                factor = near[r] * widen(jnp.exp(passed[way]), spread_half)
                held = swap_hold[way] + factor * theirs
                passed[way] = passed[way] + near[r] * log_theirs
            if r + 1 < bits:
                keep = widen(jnp.exp((1.0 - near[r]) * log_theirs), spread_half)
                take = widen(jnp.exp(near[r] * log_mine), spread_half)
                half_send[way * bits + r + 1] = (keep * mine + take * theirs).astype(bf16)
                half(r + 1).start()
                if way == 0:
                    logs(r + 1).start()
                swap_hold[way] = held
            else:
                swap_send[way] = held.astype(bf16)
                swap().start()

        def finish():
            swap().wait()
            decay = widen(jnp.exp(near[0] * log_recv[0][:, 0:NHEADS]), spread_m)
            for s in range(2):
                own = side_f if s == 1 else 1.0 - side_f
                part = own * swap_send[way].astype(f32) + (1.0 - own) * swap_recv[way].astype(f32)
                out[:, s * HALF : (s + 1) * HALF] = (
                    near[0] * full_recv[way, s].astype(f32)
                    + decay[:, s * HALF : (s + 1) * HALF] * part
                )

        def after(c):
            for r in range(min(bits, chunks)):
                pl.when(c == r)(functools.partial(step, r))

        def rest():
            for r in range(min(bits, chunks), bits):
                step(r)
            finish()

        return start, after, rest

    start, after, rest = scan_ops(0, states.at[chunks], s0)
    start()

    def rows_of(c):
        return pl.ds(pl.multiple_of(c * Q, Q), Q)

    def intra_forward(c, carry):
        rows = rows_of(c)
        in_low = act[rows, pl.ds(DI, NSTATE)].astype(bf16)
        out_low = act[rows, pl.ds(DI + NSTATE, NSTATE)].astype(bf16)
        scores = mm_nt(out_low, in_low) * lower_f
        for p in range(PAIRS):
            parts = []
            for h in (2 * p, 2 * p + 1):
                spread = cum[rows, h : h + 1] - cum_t[c, h : h + 1, :]
                parts.append((scores * jnp.exp(jnp.minimum(spread, 0.0))).astype(bf16))
            stepped = (act[rows, pair(p)] * ex_dt[rows, pair(p)].astype(f32)).astype(bf16)
            yst[rows, pair(p)] = mm(jnp.concatenate(parts, axis=1), blockdiag(stepped))
        after(c)
        return carry

    lax.fori_loop(0, chunks, intra_forward, 0)
    rest()

    sum_conv[...] = jnp.zeros_like(sum_conv)
    sum_gate[...] = jnp.zeros_like(sum_gate)
    gain_wide = gain[0:1, :]

    def state_decay(c):
        last = jnp.broadcast_to(cum_t[c][:, Q - 1 : Q], (NHEADS, 8))
        wide = jnp.concatenate([last, jnp.zeros((LANES - NHEADS, 8), f32)], axis=0)
        return wide.T[:, 0:NHEADS]

    def gating(c, before):
        rows = rows_of(c)
        decay_before = widen(jnp.exp(before), spread_m)
        out_now = act[rows, pl.ds(DI + NSTATE, NSTATE)]
        out_low = out_now.astype(bf16)
        out_t = out_now.T.astype(bf16)
        squares = jnp.zeros((Q, LANES), f32)
        for p in range(PAIRS):
            state = states[c, :, pair(p)] + decay_before[:, p * LANES : (p + 1) * LANES] * s0[
                :, pair(p)
            ]
            states[c, :, pair(p)] = state
            reached = ex_e[rows, pair(p)].astype(f32) * mm(out_low, state.astype(bf16))
            with_skip = (
                yst[rows, pair(p)]
                + reached
                + skip_wide[:, p * LANES : (p + 1) * LANES] * act[rows, pair(p)]
            )
            z = proj[rows, pair(p)].astype(f32)
            sig = sigmoid(z)
            gated = with_skip * (z * sig)
            squares += gated * gated
            yint[:, pair(p)] = reached
            ws[:, pair(p)] = with_skip
            sg[:, pair(p)] = sig
        norm = lax.rsqrt(jnp.sum(squares, axis=1, keepdims=True) * (1.0 / DI) + epsilon)
        inner = jnp.zeros((Q, LANES), f32)
        for p in range(PAIRS):
            z = proj[rows, pair(p)].astype(f32)
            gated = ws[:, pair(p)] * (z * sg[:, pair(p)])
            gain_p = gain_wide[:, p * LANES : (p + 1) * LANES]
            gate_low[rows, pair(p)] = (gated * norm * gain_p).astype(bf16)
            inner += grad_low[rows, pair(p)] * gain_p * gated
            sum_gate[0:8, pair(p)] += fold_rows(grad_low[rows, pair(p)] * (gated * norm))
        mean = jnp.sum(inner, axis=1, keepdims=True) * (1.0 / DI)
        pull = norm * norm * norm * mean
        later = jnp.zeros((Q, NHEADS), f32)
        for p in range(PAIRS):
            z = proj[rows, pair(p)].astype(f32)
            sig = sg[:, pair(p)]
            with_skip = ws[:, pair(p)]
            gain_p = gain_wide[:, p * LANES : (p + 1) * LANES]
            gated = with_skip * (z * sig)
            grad_gated = norm * (grad_low[rows, pair(p)] * gain_p) - gated * pull
            grad = grad_gated * (z * sig)
            gs[rows, pair(p)] = grad
            grad_z = grad_gated * with_skip * (sig * (1.0 + z * (1.0 - sig)))
            grad_proj[rows, pair(p)] = grad_z.astype(bf16)
            sum_gate[8:16, pair(p)] += fold_rows(grad * act[rows, pair(p)])
            later += mm((grad * yint[:, pair(p)]).astype(bf16), gather_m(p))
            scaled = (grad * ex_e[rows, pair(p)].astype(f32)).astype(bf16)
            adjs[c, :, pair(p)] = mm(out_t, scaled)
        grad_a[rows, :] = mm_exact(upper_f, later)
        return before + state_decay(c)

    lax.fori_loop(0, chunks, gating, jnp.zeros((8, NHEADS), f32))

    adjs[chunks] = jnp.zeros((NSTATE, DI), f32)

    def local_adjoints(i, carry):
        c = chunks - 1 - i
        decay = widen(jnp.exp(state_decay(c)), spread_m)
        for p in range(PAIRS):
            adjs[c, :, pair(p)] = (
                decay[:, p * LANES : (p + 1) * LANES] * adjs[c + 1, :, pair(p)]
                + adjs[c, :, pair(p)]
            )
        return carry

    lax.fori_loop(0, chunks, local_adjoints, 0)
    start, after, rest = scan_ops(1, adjs.at[0], g0)
    start()

    def intra_backward(c, carry):
        rows = rows_of(c)
        in_low = act[rows, pl.ds(DI, NSTATE)].astype(bf16)
        out_low = act[rows, pl.ds(DI + NSTATE, NSTATE)].astype(bf16)
        scores = mm_nt(in_low, out_low) * upper_f
        grad_scores = jnp.zeros((Q, Q), f32)
        tails = upper_f.T.astype(bf16)
        found = []
        for p in range(PAIRS):
            grad = gs[rows, pair(p)].astype(bf16)
            stepped = (act[rows, pair(p)] * ex_dt[rows, pair(p)].astype(f32)).astype(bf16)
            values = mm_nt(blockdiag(stepped), grad)
            weights, crosses = [], []
            for i, h in enumerate((2 * p, 2 * p + 1)):
                spread = cum_t[c, h : h + 1, :] - cum[rows, h : h + 1]
                decays = jnp.exp(jnp.minimum(spread, 0.0))
                weights.append((scores * decays).astype(bf16))
                part = decays * values[i * Q : (i + 1) * Q, :]
                grad_scores += part
                crosses.append((part * scores).astype(bf16))
            yst[rows, pair(p)] = mm(jnp.concatenate(weights, axis=1), blockdiag(grad))
            sums = mm(jnp.concatenate(crosses, axis=0), tails)
            for i in range(2):
                picked = jnp.where(strict_upper, sums[i * Q : (i + 1) * Q, :], 0.0)
                found.append(jnp.sum(picked, axis=0, keepdims=True))
        found.append(jnp.zeros((LANES - NHEADS, Q), f32))
        grad_a[rows, :] += jnp.concatenate(found, axis=0).T[:, 0:NHEADS]
        grad_low_scores = (grad_scores * upper_f).astype(bf16)
        gpad[rows, pl.ds(DI, NSTATE)] = mm(grad_low_scores, out_low)
        gpad[rows, pl.ds(DI + NSTATE, NSTATE)] = mm((grad_scores * upper_f).T.astype(bf16), in_low)
        after(c)
        return carry

    lax.fori_loop(0, chunks, intra_backward, 0)
    rest()

    sum_head[...] = jnp.zeros_like(sum_head)

    def finish_backward(c, before):
        after_log = jnp.broadcast_to(log_total, (8, NHEADS)) - before - state_decay(c)
        decay_after = widen(jnp.exp(after_log), spread_m)
        rows = rows_of(c)
        in_low = act[rows, pl.ds(DI, NSTATE)].astype(bf16)
        grad_in = gpad[rows, pl.ds(DI, NSTATE)]
        grad_out = gpad[rows, pl.ds(DI + NSTATE, NSTATE)]
        kept = jnp.zeros((Q, NHEADS), f32)
        grad_step = jnp.zeros((Q, NHEADS), f32)
        crossing = jnp.zeros((8, NHEADS), f32)
        for p in range(PAIRS):
            adj = adjs[c + 1, :, pair(p)] + decay_after[:, p * LANES : (p + 1) * LANES] * g0[
                :, pair(p)
            ]
            adj_low = adj.astype(bf16)
            state = states[c, :, pair(p)]
            x = act[rows, pair(p)]
            dt = ex_dt[rows, pair(p)].astype(f32)
            to_end = ex_f[rows, pair(p)].astype(f32)
            grad = gs[rows, pair(p)]
            later = to_end * mm(in_low, adj_low)
            total = yst[rows, pair(p)] + later
            stepped = x * dt
            pick = gather_m(p)
            kept += mm((stepped * later).astype(bf16), pick)
            grad_step += mm((x * total).astype(bf16), pick)
            crossing += mm(fold_rows(adj * state).astype(bf16), pick)
            grad_in += mm_nt((stepped * to_end).astype(bf16), adj_low)
            scaled = (grad * ex_e[rows, pair(p)].astype(f32)).astype(bf16)
            grad_out += mm_nt(scaled, state.astype(bf16))
            grad_x = dt * total + skip_wide[:, p * LANES : (p + 1) * LANES] * grad
            gpad[rows, pair(p)] = grad_x * dsilu[rows, pair(p)]
        gpad[rows, pl.ds(DI, NSTATE)] = grad_in * dsilu[rows, pl.ds(DI, NSTATE)]
        gpad[rows, pl.ds(DI + NSTATE, NSTATE)] = grad_out * dsilu[rows, pl.ds(DI + NSTATE, NSTATE)]
        whole = jnp.exp(state_decay(c))[0:1, :] * jnp.sum(crossing, axis=0, keepdims=True)
        grad_decay = grad_a[rows, :] + mm_exact(lower_f - upper_f * lower_f, kept) + whole
        grad_raw = (grad_step - rate * grad_decay) * sgm[rows, :]
        grad_proj[rows, pl.ds(DI + DC, NHEADS)] = grad_raw.astype(bf16)
        sum_head[0:8, 0:NHEADS] += fold_rows(grad_raw)
        sum_head[8:16, 0:NHEADS] += fold_rows(grad_decay * logd[rows, :])

        @pl.when(jnp.logical_and(c == 0, me > 0))
        def _():
            grad_edge_copy().start()

        return before + state_decay(c)

    lax.fori_loop(0, chunks, finish_backward, jnp.zeros((8, NHEADS), f32))

    @pl.when(me > 0)
    def _():
        grad_edge_copy().wait_send()

    @pl.when(me < seq_size - 1)
    def _():
        grad_edge_copy().wait_recv()
        gpad[pl.ds(length, 8), :] = grad_edge[...]

    @pl.when(me == seq_size - 1)
    def _():
        gpad[pl.ds(length, 8), :] = jnp.zeros((8, DC), f32)

    def conv_backward(c, carry):
        rows = rows_of(c)
        longer = pl.ds(pl.multiple_of(c * Q, Q), Q + 8)
        for block in range(DC // LANES):
            lanes = pl.ds(block * LANES, LANES)
            grads = gpad[longer, lanes]
            inputs = cpad[longer, lanes]
            grad = grads[0:Q, :]
            grad_conv = sum(
                taps[k : k + 1, lanes] * grads[KCONV - 1 - k : KCONV - 1 - k + Q, :]
                for k in range(KCONV)
            )
            grad_proj[rows, pl.ds(DI + block * LANES, LANES)] = grad_conv.astype(bf16)
            for k in range(KCONV):
                sum_conv[8 * k : 8 * k + 8, lanes] += fold_rows(grad * inputs[5 + k : 5 + k + Q, :])
            sum_conv[8 * KCONV : 8 * KCONV + 8, lanes] += fold_rows(grad)
        return carry

    lax.fori_loop(0, chunks, conv_backward, 0)


def ssd_call(seq_size, proj, grad_low, taps, cbias, heads, gain):
    length = proj.shape[0]
    chunks = length // Q
    bits = seq_size.bit_length() - 1
    vmem = lambda shape, kind=f32: pltpu.VMEM(shape, kind)
    space = pl.BlockSpec(memory_space=pltpu.VMEM)
    return pl.pallas_call(
        functools.partial(ssd_kernel, seq_size),
        name="ssd",
        out_shape=(
            jax.ShapeDtypeStruct((length, DI), bf16),
            jax.ShapeDtypeStruct((length, proj.shape[1]), bf16),
            jax.ShapeDtypeStruct((8 * (KCONV + 1), DC), f32),
            jax.ShapeDtypeStruct((16, DI), f32),
            jax.ShapeDtypeStruct((16, LANES), f32),
        ),
        in_specs=[space] * 6,
        out_specs=[space] * 5,
        scratch_shapes=[
            vmem((length + 8, DC)),
            vmem((length, DC)),
            vmem((length, DC)),
            vmem((length + 8, DC)),
            vmem((Q, DI)),
            vmem((length, DI)),
            vmem((Q, DI)),
            vmem((Q, DI)),
            vmem((length, DI)),
            vmem((length, DI), bf16),
            vmem((length, DI), bf16),
            vmem((length, DI), bf16),
            vmem((length, NHEADS)),
            vmem((chunks, NHEADS, Q)),
            vmem((length, NHEADS)),
            vmem((length, NHEADS)),
            vmem((length, NHEADS)),
            vmem((length, NHEADS)),
            vmem((chunks + 1, NSTATE, DI)),
            vmem((chunks + 1, NSTATE, DI)),
            vmem((NSTATE, DI)),
            vmem((NSTATE, DI)),
            vmem((16, DC), bf16),
            vmem((8, DC)),
            vmem((2, 2, NSTATE, HALF), bf16),
            vmem((2, 2, NSTATE, HALF), bf16),
            vmem((2 * bits, NSTATE, HALF), bf16),
            vmem((2 * bits, NSTATE, HALF), bf16),
            vmem((2, NSTATE, HALF), bf16),
            vmem((2, NSTATE, HALF), bf16),
            vmem((bits, 8, LANES)),
            vmem((bits, 8, LANES)),
            pltpu.SemaphoreType.DMA((4,)),
            pltpu.SemaphoreType.DMA((2, 2)),
            pltpu.SemaphoreType.DMA((2 * bits, 2)),
            pltpu.SemaphoreType.DMA((2, 2)),
            pltpu.SemaphoreType.DMA((bits, 2)),
            vmem((2, NSTATE, HALF)),
            vmem((2, 8, NHEADS)),
        ],
        compiler_params=pltpu.CompilerParams(
            collective_id=1, has_side_effects=True, vmem_limit_bytes=62 * 1024 * 1024
        ),
    )(proj, grad_low, taps, cbias, heads, gain)


def mesh_digits(sizes):
    steps = [("seq", 1 << r, 2) for r in range(sizes["seq"].bit_length() - 1)]
    first = [("dp", 1, sizes["dp"])]
    return first + steps[1:] + steps[:1], first + steps[:0:-1] + steps[:1]


def digit_of(digit):
    axis, stride, size = digit
    return (lax.axis_index(axis) // stride) % size


def moved(digit, offset):
    axis, stride, size = digit
    now = digit_of(digit)
    return lax.axis_index(axis) + ((now + offset) % size - now) * stride


def rank_at(sizes, changes):
    place = {axis: lax.axis_index(axis) for axis in sizes}
    for digit, offset in changes:
        axis, stride, size = digit
        now = digit_of(digit)
        place[axis] = place[axis] + ((now + offset) % size - now) * stride
    return place["dp"] * sizes["seq"] + place["seq"]


def greet(sizes):
    barrier = pltpu.get_barrier_semaphore()
    count = 0
    for digit in mesh_digits(sizes)[0]:
        for offset in range(1, digit[2]):
            pl.semaphore_signal(
                barrier, inc=1, device_id={digit[0]: moved(digit, offset)}, device_id_type=MESH
            )
            count += 1
    pl.semaphore_wait(barrier, count)


def spans(width, parts):
    tiles = width // LANES
    edges = [tiles * k // parts * LANES for k in range(parts)] + [width]
    return [(edges[k], edges[k + 1] - edges[k]) for k in range(parts)]


def gather_kernel(sizes, *refs):
    items = 3
    sources, targets = refs[:items], refs[items : 2 * items]
    own_sems, sends, arrivals = refs[2 * items :]
    greet(sizes)
    orders = mesh_digits(sizes)
    mine = rank_at(sizes, [])
    for k in range(items):
        pltpu.make_async_copy(sources[k], targets[k].at[mine], own_sems.at[k]).start()

    streams = []
    for k in range(items):
        width = sources[k].shape[1]
        for j, (at, size) in enumerate(spans(width, 2 if width > 512 else 1)):
            streams.append((k, at, size, orders[j], len(streams)))
    used = [0] * len(streams)
    waits = []

    def copy(stream, changes, digit, offset, first):
        k, at, size, _, index = stream
        slot = rank_at(sizes, changes)
        lanes = pl.ds(at, size)
        source = sources[k].at[:, lanes] if first else targets[k].at[slot, :, lanes]
        return pltpu.make_async_remote_copy(
            src_ref=source,
            dst_ref=targets[k].at[slot, :, lanes],
            send_sem=sends.at[index, used[index]],
            recv_sem=arrivals.at[index, slot],
            device_id={digit[0]: moved(digit, offset)},
            device_id_type=MESH,
        )

    def pass_on(stream, changes, depth):
        order = stream[3]
        for position in range(depth, len(order)):
            digit = order[position]
            for offset in range(1, digit[2]):
                started = copy(stream, changes, digit, offset, not changes)
                used[stream[4]] += 1
                started.start()
                waits.append(started)

    def arrived(stream, changes):
        k, at, size, _, index = stream
        slot = rank_at(sizes, changes)
        lanes = pl.ds(at, size)
        pltpu.make_async_remote_copy(
            src_ref=targets[k].at[slot, :, lanes],
            dst_ref=targets[k].at[slot, :, lanes],
            send_sem=sends.at[index, 0],
            recv_sem=arrivals.at[index, slot],
            device_id={"dp": moved(orders[0][0], 1)},
            device_id_type=MESH,
        ).wait_recv()

    def shards(order, depth):
        found = [[]]
        for position in range(depth):
            found = [
                held + ([(order[position], offset)] if offset else [])
                for held in found
                for offset in range(order[position][2])
            ]
        return [
            held + [(order[depth], offset)] for held in found for offset in range(1, order[depth][2])
        ]

    for stream in streams:
        pass_on(stream, [], 0)
    for depth in range(len(orders[0])):
        lists = [(stream, shards(stream[3], depth)) for stream in streams]
        for turn in range(len(lists[0][1])):
            for stream, held in lists:
                arrived(stream, held[turn])
                pass_on(stream, held[turn], depth + 1)
    for started in waits:
        started.wait_send()
    for k in range(items):
        pltpu.make_async_copy(sources[k], targets[k].at[mine], own_sems.at[k]).wait()


def gather_call(sizes, *arrays):
    count = sizes["dp"] * sizes["seq"]
    streams = 5
    return pl.pallas_call(
        functools.partial(gather_kernel, sizes),
        name="gather",
        out_shape=tuple(jax.ShapeDtypeStruct((count,) + a.shape, a.dtype) for a in arrays),
        in_specs=[pl.BlockSpec(memory_space=pltpu.VMEM)] * len(arrays),
        out_specs=[pl.BlockSpec(memory_space=pl.ANY)] * len(arrays),
        scratch_shapes=[
            pltpu.SemaphoreType.DMA((len(arrays),)),
            pltpu.SemaphoreType.DMA((streams, count)),
            pltpu.SemaphoreType.DMA((streams, count)),
        ],
        compiler_params=pltpu.CompilerParams(collective_id=2, has_side_effects=True),
    )(*arrays)


def scatter_kernel(sizes, parts, items, *refs):
    orders = mesh_digits(sizes)
    depth = len(orders[0])
    lengths = [digit[2] for digit in orders[0]]
    counts = [1]
    for size in lengths:
        counts.append(counts[-1] * size)
    sources, refs = refs[:items], refs[items:]
    targets, refs = refs[:items], refs[items:]
    sums, refs = refs[:items], refs[items:]
    landed, refs = refs[: items * depth], refs[items * depth :]
    sends, arrivals = refs
    greet(sizes)

    streams = []
    for k in range(items):
        for j, (at, size) in enumerate(spans(sources[k].shape[2], parts[k])):
            streams.append((k, pl.ds(at, size), orders[j % 2], len(streams)))
    base = [0]
    for position in range(depth):
        base.append(base[-1] + (lengths[position] - 1) * counts[position])
    started, waiting = [], []

    def offsets_of(relative):
        found = []
        for size in lengths:
            found.append(relative % size)
            relative //= size
        return found

    def copy(stream, position, offset, relative):
        k, lanes, order, index = stream
        digit = order[position]
        if position == depth - 1:
            changes = list(zip(order, offsets_of(relative) [:position] + [offset]))
            source = sources[k].at[rank_at(sizes, changes), :, lanes]
        else:
            source = sums[k].at[offset * counts[position] + relative, :, lanes]
        there = (digit[2] - offset - 1) * counts[position] + relative
        return pltpu.make_async_remote_copy(
            src_ref=source,
            dst_ref=landed[k * depth + position].at[there, :, lanes],
            send_sem=sends.at[index, base[position] + there],
            recv_sem=arrivals.at[index, base[position] + there],
            device_id={digit[0]: moved(digit, offset)},
            device_id_type=MESH,
        )

    def flush(keep):
        while len(waiting) > keep:
            item = waiting.pop(0)
            item.start()
            started.append(item)

    def receive(stream, position, relative):
        k, lanes, order, index = stream
        if position == depth - 1:
            own = list(zip(order, offsets_of(relative)[:position]))
            total = sources[k][rank_at(sizes, own), :, lanes].astype(f32)
        else:
            total = sums[k][relative, :, lanes].astype(f32)
        buffer = landed[k * depth + position]
        for offset in range(1, lengths[position]):
            here = (offset - 1) * counts[position] + relative
            pltpu.make_async_remote_copy(
                src_ref=buffer.at[here, :, lanes],
                dst_ref=buffer.at[here, :, lanes],
                send_sem=sends.at[index, base[position] + here],
                recv_sem=arrivals.at[index, base[position] + here],
                device_id={order[position][0]: moved(order[position], offset)},
                device_id_type=MESH,
            ).wait_recv()
            total += buffer[here, :, lanes].astype(f32)
        if position == 0:
            targets[k][:, lanes] = total
            return
        sums[k][relative, :, lanes] = total.astype(sums[k].dtype)
        offset, below = divmod(relative, counts[position - 1])
        if offset:
            waiting.append(copy(stream, position - 1, offset, below))

    for relative in reversed(range(counts[depth - 1])):
        for stream in streams:
            for offset in range(1, lengths[depth - 1]):
                waiting.append(copy(stream, depth - 1, offset, relative))
                flush(0)
    for position in reversed(range(depth)):
        for relative in reversed(range(counts[position])):
            for stream in streams:
                receive(stream, position, relative)
                flush(1)
        flush(0)
    for item in started:
        item.wait_send()


def scatter_call(sizes, parts, *arrays):
    depth = sizes["seq"].bit_length()
    lengths = [sizes["dp"]] + [2] * (depth - 1)
    counts = [1]
    for size in lengths:
        counts.append(counts[-1] * size)
    most = sum((lengths[j] - 1) * counts[j] for j in range(depth))
    scratch = [pltpu.VMEM((counts[depth - 1],) + a.shape[1:], a.dtype) for a in arrays]
    for a in arrays:
        for j in range(depth):
            scratch.append(pltpu.VMEM(((lengths[j] - 1) * counts[j],) + a.shape[1:], a.dtype))
    return pl.pallas_call(
        functools.partial(scatter_kernel, sizes, parts, len(arrays)),
        name="scatter",
        out_shape=tuple(jax.ShapeDtypeStruct(a.shape[1:], f32) for a in arrays),
        in_specs=[pl.BlockSpec(memory_space=pltpu.VMEM)] * len(arrays),
        out_specs=[pl.BlockSpec(memory_space=pltpu.VMEM)] * len(arrays),
        scratch_shapes=scratch
        + [
            pltpu.SemaphoreType.DMA((sum(parts), most)),
            pltpu.SemaphoreType.DMA((sum(parts), most)),
        ],
        compiler_params=pltpu.CompilerParams(
            collective_id=3, has_side_effects=True, vmem_limit_bytes=62 * 1024 * 1024
        ),
    )(*arrays)


def rms_scale(values, weight):
    return values * lax.rsqrt(jnp.mean(values * values, axis=-1, keepdims=True) + epsilon) * weight


def local(
    dp_size,
    seq_size,
    tokens,
    cotangent,
    norm_gain,
    in_weight,
    conv_weight,
    conv_bias,
    dt_bias,
    a_log,
    d_skip,
    gate_gain,
    out_weight,
):
    axes = ("dp", "seq")
    sizes = [norm_gain.shape[0], conv_weight.size, conv_bias.shape[0], gate_gain.shape[0]]
    packed = jnp.concatenate([norm_gain, conv_weight.reshape(-1), conv_bias, gate_gain])
    in_full, out_full, packed = gather_call(
        {"dp": dp_size, "seq": seq_size}, in_weight, out_weight, packed[None].astype(f32)
    )
    in_full = in_full.reshape(-1, in_weight.shape[1])
    out_full = out_full.reshape(-1, out_weight.shape[1])
    packed = packed[:, 0]
    offsets = [0]
    for size in sizes:
        offsets.append(offsets[-1] + size)
    norm_full = packed[:, : offsets[1]].reshape(-1)
    taps_full = packed[:, offsets[1] : offsets[2]].reshape(-1, KCONV, conv_weight.shape[1])
    taps_full = jnp.swapaxes(taps_full, 0, 1).reshape(KCONV, DC)
    cbias_full = packed[:, offsets[2] : offsets[3]].reshape(1, DC)
    gain_full = packed[:, offsets[3] :].reshape(1, DI)
    heads = jnp.stack([dt_bias, a_log, d_skip])

    tokens = tokens[0]
    cotangent = cotangent[0]
    inputs = tokens.astype(f32)
    normed, norm_back = jax.vjp(rms_scale, inputs, norm_full)
    normed_low = normed.astype(bf16)
    proj = mm(normed_low, in_full).astype(bf16)
    grad_low = mm_nt(cotangent, out_full)
    gate_low, grad_proj, sum_conv, sum_gate, sum_head = ssd_call(
        seq_size, proj, grad_low, taps_full, cbias_full, heads, gain_full
    )
    block_out = (inputs + mm(gate_low, out_full)).astype(bf16)
    outward = lax.dot_general(
        gate_low, cotangent, (((0,), (0,)), ((), ())), preferred_element_type=f32
    )
    inward = lax.dot_general(
        normed_low, grad_proj, (((0,), (0,)), ((), ())), preferred_element_type=f32
    )
    grad_normed = mm_nt(grad_proj, in_full)
    grad_inputs, norm_local = norm_back(grad_normed)
    input_grad = (grad_inputs + cotangent.astype(f32)).astype(bf16)

    conv_local = jnp.sum(sum_conv.reshape(KCONV + 1, 8, DC), axis=1)
    gate_local = jnp.sum(sum_gate.reshape(2, 8, DI), axis=1)
    head_local = jnp.sum(sum_head.reshape(2, 8, LANES), axis=1)[:, :NHEADS]
    skip_local = jnp.sum(gate_local[1].reshape(NHEADS, HEADDIM), axis=1)
    count = dp_size * seq_size
    shared = jnp.concatenate([head_local.reshape(-1), skip_local])
    pieces = [
        norm_local.reshape(count, -1),
        jnp.swapaxes(conv_local[:KCONV].reshape(KCONV, count, -1), 0, 1).reshape(count, -1),
        conv_local[KCONV].reshape(count, -1),
        gate_local[0].reshape(count, -1),
        jnp.broadcast_to(shared[None], (count, shared.shape[0])),
    ]
    widths = [piece.shape[1] for piece in pieces]
    width = -(-sum(widths) // LANES) * LANES
    pieces.append(jnp.zeros((count, width - sum(widths)), f32))
    inward, outward, small = scatter_call(
        {"dp": dp_size, "seq": seq_size},
        (4, 2, 1),
        inward.astype(bf16).reshape(count, -1, inward.shape[1]),
        outward.astype(bf16).reshape(count, -1, outward.shape[1]),
        jnp.concatenate(pieces, axis=1)[:, None],
    )
    at = [sum(widths[:k]) for k in range(6)]
    parts = [small[0, at[k] : at[k + 1]] for k in range(5)]
    norm_grad, kernel_grad, offset_grad, gain_grad, shared = parts
    kernel_grad = kernel_grad.reshape(KCONV, -1)
    step_grad, decay_grad, skip_grad = shared.reshape(3, NHEADS)
    return (
        block_out[None],
        input_grad[None],
        norm_grad,
        inward,
        kernel_grad,
        offset_grad,
        step_grad,
        decay_grad,
        skip_grad,
        gain_grad,
        outward,
    )


def solution(mesh):
    both = ("dp", "seq")
    return jax.shard_map(
        functools.partial(local, mesh.shape["dp"], mesh.shape["seq"]),
        mesh=mesh,
        in_specs=(
            P("dp", "seq", None),
            P("dp", "seq", None),
            P(both),
            P(both, None),
            P(None, both),
            P(both),
            P(),
            P(),
            P(),
            P(both),
            P(both, None),
        ),
        out_specs=(
            P("dp", "seq", None),
            P("dp", "seq", None),
            P(both),
            P(both, None),
            P(None, both),
            P(both),
            P(),
            P(),
            P(),
            P(both),
            P(both, None),
        ),
        check_vma=False,
    )
```

```python
import functools

import jax
import jax.numpy as jnp
from jax import lax
from jax.experimental import pallas as pl
from jax.experimental.pallas import tpu as pltpu
from jax.sharding import PartitionSpec as P

MESH = pl.DeviceIdType.MESH
NHEADS = 24
HEADDIM = 64
NSTATE = 128
KCONV = 4
DI = 1536
DC = 1792
Q = 128
LANES = 128
PAIRS = DI // LANES
HALF = DI // 2
epsilon = 1e-05
highest = lax.Precision.HIGHEST
f32 = jnp.float32
bf16 = jnp.bfloat16


def mm(a, b):
    return lax.dot_general(a, b, (((1,), (0,)), ((), ())), preferred_element_type=f32)


def mm_nt(a, b):
    return lax.dot_general(a, b, (((1,), (1,)), ((), ())), preferred_element_type=f32)


def mm_exact(a, b):
    return lax.dot_general(
        a, b, (((1,), (0,)), ((), ())), precision=highest, preferred_element_type=f32
    )


def sigmoid(v):
    return 1.0 / (1.0 + jnp.exp(-v))


def fold_rows(v):
    return jnp.sum(v.reshape(v.shape[0] // 8, 8, v.shape[1]), axis=0)


def ssd_kernel(
    seq_size,
    proj,
    grad_low,
    taps,
    cbias,
    heads,
    gain,
    gate_low,
    grad_proj,
    sum_conv,
    sum_gate,
    sum_head,
    cpad,
    act,
    dsilu,
    gpad,
    yint,
    yst,
    ws,
    sg,
    gs,
    ex_e,
    ex_f,
    ex_dt,
    cum,
    cum_t,
    dts,
    logd,
    sgm,
    grad_a,
    states,
    adjs,
    s0,
    g0,
    conv_edge,
    grad_edge,
    full_send,
    full_recv,
    half_send,
    half_recv,
    swap_send,
    swap_recv,
    log_send,
    log_recv,
    edge_sems,
    full_sems,
    half_sems,
    swap_sems,
    log_sems,
    swap_hold,
    passed,
):
    length = proj.shape[0]
    chunks = length // Q
    me = lax.axis_index("seq")
    bits = seq_size.bit_length() - 1
    bit = [(me // (1 << r)) % 2 for r in range(bits)]
    partner = [me + (1 - 2 * bit[r]) * (1 << r) for r in range(bits)]
    side = bit[0]

    barrier = pltpu.get_barrier_semaphore()
    for other in partner:
        pl.semaphore_signal(barrier, inc=1, device_id={"seq": other}, device_id_type=MESH)

    @pl.when(me > 0)
    def _():
        pl.semaphore_signal(barrier, inc=1, device_id={"seq": me - 1}, device_id_type=MESH)

    @pl.when(me < seq_size - 1)
    def _():
        pl.semaphore_signal(barrier, inc=1, device_id={"seq": me + 1}, device_id_type=MESH)

    pl.semaphore_wait(barrier, bits + jnp.where(me > 0, 1, 0) + jnp.where(me < seq_size - 1, 1, 0))

    def edge_copy():
        return pltpu.make_async_remote_copy(
            src_ref=proj.at[pl.ds(length - 16, 16), pl.ds(DI, DC)],
            dst_ref=conv_edge,
            send_sem=edge_sems.at[0],
            recv_sem=edge_sems.at[1],
            device_id={"seq": me + 1},
            device_id_type=MESH,
        )

    def grad_edge_copy():
        return pltpu.make_async_remote_copy(
            src_ref=gpad.at[pl.ds(0, 8), :],
            dst_ref=grad_edge,
            send_sem=edge_sems.at[2],
            recv_sem=edge_sems.at[3],
            device_id={"seq": me - 1},
            device_id_type=MESH,
        )

    def exchange(src, dst, sems, index, other):
        return pltpu.make_async_remote_copy(
            src_ref=src,
            dst_ref=dst,
            send_sem=sems.at[index, 0],
            recv_sem=sems.at[index, 1],
            device_id={"seq": other},
            device_id_type=MESH,
        )

    @pl.when(me < seq_size - 1)
    def _():
        edge_copy().start()

    lane_head = lax.broadcasted_iota(jnp.int32, (NHEADS, DI), 1) // HEADDIM
    spread_m = (lane_head == lax.broadcasted_iota(jnp.int32, (NHEADS, DI), 0)).astype(bf16)
    rows_i = lax.broadcasted_iota(jnp.int32, (Q, Q), 0)
    cols_i = lax.broadcasted_iota(jnp.int32, (Q, Q), 1)
    lower = (rows_i >= cols_i)
    lower_f = lower.astype(f32)
    upper_f = (rows_i <= cols_i).astype(f32)
    strict_upper = rows_i < cols_i
    low_lane = lax.broadcasted_iota(jnp.int32, (Q, LANES), 1) < HEADDIM

    def gather_m(p):
        lane = lax.broadcasted_iota(jnp.int32, (LANES, NHEADS), 0) // HEADDIM + 2 * p
        return (lane == lax.broadcasted_iota(jnp.int32, (LANES, NHEADS), 1)).astype(bf16)

    def pair(p):
        return pl.ds(p * LANES, LANES)

    def blockdiag(v):
        zero = jnp.zeros_like(v)
        return jnp.concatenate([jnp.where(low_lane, v, zero), jnp.where(low_lane, zero, v)], axis=0)

    def spread_row(row):
        hi = row.astype(bf16)
        rest = row - hi.astype(f32)
        mid = rest.astype(bf16)
        lo = (rest - mid.astype(f32)).astype(bf16)
        return mm(hi, spread_m) + mm(mid, spread_m) + mm(lo, spread_m)

    dt_bias = heads[0:1, :]
    rate = jnp.exp(heads[1:2, :])
    skip_wide = spread_row(jnp.broadcast_to(heads[2:3, :], (8, NHEADS)))[0:1, :]

    def rates(c, carry):
        rows = pl.ds(pl.multiple_of(c * Q, Q), Q)
        raw = proj[rows, pl.ds(DI + DC, NHEADS)].astype(f32) + dt_bias
        dt = jnp.maximum(raw, 0.0) + jnp.log1p(jnp.exp(-jnp.abs(raw)))
        ld = -dt * rate
        run = mm_exact(lower_f, ld)
        dts[rows, :] = dt
        logd[rows, :] = ld
        sgm[rows, :] = sigmoid(raw)
        cum[rows, :] = run
        wide = jnp.concatenate([run, jnp.zeros((Q, LANES - NHEADS), f32)], axis=1)
        cum_t[c] = wide.T[0:NHEADS, :]
        last = run[Q - 1 : Q, :]
        ex_e[rows, :] = mm(jnp.exp(run).astype(bf16), spread_m).astype(bf16)
        ex_f[rows, :] = mm(jnp.exp(last - run).astype(bf16), spread_m).astype(bf16)
        ex_dt[rows, :] = mm(dt.astype(bf16), spread_m).astype(bf16)
        return carry + last

    log_total = lax.fori_loop(0, chunks, rates, jnp.zeros((1, NHEADS), f32))

    def load_conv(c, carry):
        rows = pl.ds(pl.multiple_of(c * Q, Q), Q)
        cpad[pl.ds(pl.multiple_of(c * Q + 8, 8), Q), :] = proj[rows, pl.ds(DI, DC)].astype(f32)
        return carry

    lax.fori_loop(0, chunks, load_conv, 0)

    @pl.when(me > 0)
    def _():
        edge_copy().wait_recv()
        cpad[0:8, :] = conv_edge[...].astype(f32)[8:16, :]

    @pl.when(me == 0)
    def _():
        cpad[0:8, :] = jnp.zeros((8, DC), f32)

    @pl.when(me < seq_size - 1)
    def _():
        edge_copy().wait_send()

    def conv_block(c, block):
        lanes = pl.ds(block * LANES, LANES)
        window = cpad[pl.ds(pl.multiple_of(c * Q, Q), Q + 8), lanes]
        pre = cbias[0:1, lanes] + sum(
            taps[k : k + 1, lanes] * window[5 + k : 5 + k + Q, :] for k in range(KCONV)
        )
        gate = sigmoid(pre)
        value = pre * gate
        rows = pl.ds(pl.multiple_of(c * Q, Q), Q)
        act[rows, lanes] = value
        dsilu[rows, lanes] = gate + value * (1.0 - gate)

    def local_states(c, carry):
        rows = pl.ds(pl.multiple_of(c * Q, Q), Q)
        for block in range(DC // LANES):
            conv_block(c, block)
        decay = spread_row(jnp.exp(jnp.broadcast_to(cum_t[c][:, Q - 1 : Q], (NHEADS, 8)).T))[0:1, :]
        in_t = act[rows, pl.ds(DI, NSTATE)].T.astype(bf16)
        for p in range(PAIRS):
            xw = act[rows, pair(p)] * (ex_f[rows, pair(p)].astype(f32) * ex_dt[rows, pair(p)].astype(f32))
            states[c + 1, :, pair(p)] = decay[:, p * LANES : (p + 1) * LANES] * states[
                c, :, pair(p)
            ] + mm(in_t, xw.astype(bf16))
        return carry

    states[0] = jnp.zeros((NSTATE, DI), f32)
    lax.fori_loop(0, chunks, local_states, 0)

    log_send[0] = jnp.concatenate(
        [jnp.broadcast_to(log_total, (8, NHEADS)), jnp.zeros((8, LANES - NHEADS), f32)], axis=1
    )


    side_f = side.astype(f32)
    half_lane = (lax.broadcasted_iota(jnp.int32, (NHEADS, HALF), 1) + side * HALF) // HEADDIM
    spread_half = (half_lane == lax.broadcasted_iota(jnp.int32, (NHEADS, HALF), 0)).astype(bf16)

    def widen(row, matrix):
        hi = row.astype(bf16)
        rest = row - hi.astype(f32)
        mid = rest.astype(bf16)
        return (mm(hi, matrix) + mm(mid, matrix))[0:1, :]

    def scan_ops(way, total, out):
        near = [(bit[r] if way == 0 else 1 - bit[r]).astype(f32) for r in range(bits)]

        def full():
            return exchange(full_send.at[way], full_recv.at[way], full_sems, way, partner[0])

        def half(r):
            k = way * bits + r
            return exchange(half_send.at[k], half_recv.at[k], half_sems, k, partner[r])

        def swap():
            return exchange(swap_send.at[way], swap_recv.at[way], swap_sems, way, partner[0])

        def logs(r):
            return exchange(log_send.at[r], log_recv.at[r], log_sems, r, partner[r])

        def start():
            for s in range(2):
                full_send[way, s] = total[:, s * HALF : (s + 1) * HALF].astype(bf16)
            full().start()
            if way == 0:
                logs(0).start()
            passed[way] = jnp.zeros((8, NHEADS), f32)

        def step(r):
            if r == 0:
                full().wait()
            else:
                half(r).wait()
            if way == 0:
                logs(r).wait()
                if r + 1 < bits:
                    log_send[r + 1] = log_send[r] + log_recv[r]
            log_mine = log_send[r][:, 0:NHEADS]
            log_theirs = log_recv[r][:, 0:NHEADS]
            if r == 0:
                mine = full_send[way, side].astype(f32)
                theirs = full_recv[way, side].astype(f32)
                held = jnp.zeros((NSTATE, HALF), f32)
            else:
                mine = half_send[way * bits + r].astype(f32)
                theirs = half_recv[way * bits + r].astype(f32)
                factor = near[r] * widen(jnp.exp(passed[way]), spread_half)
                held = swap_hold[way] + factor * theirs
                passed[way] = passed[way] + near[r] * log_theirs
            if r + 1 < bits:
                keep = widen(jnp.exp((1.0 - near[r]) * log_theirs), spread_half)
                take = widen(jnp.exp(near[r] * log_mine), spread_half)
                half_send[way * bits + r + 1] = (keep * mine + take * theirs).astype(bf16)
                half(r + 1).start()
                if way == 0:
                    logs(r + 1).start()
                swap_hold[way] = held
            else:
                swap_send[way] = held.astype(bf16)
                swap().start()

        def finish():
            swap().wait()
            decay = widen(jnp.exp(near[0] * log_recv[0][:, 0:NHEADS]), spread_m)
            for s in range(2):
                own = side_f if s == 1 else 1.0 - side_f
                part = own * swap_send[way].astype(f32) + (1.0 - own) * swap_recv[way].astype(f32)
                out[:, s * HALF : (s + 1) * HALF] = (
                    near[0] * full_recv[way, s].astype(f32)
                    + decay[:, s * HALF : (s + 1) * HALF] * part
                )

        def after(c):
            for r in range(min(bits, chunks)):
                pl.when(c == r)(functools.partial(step, r))

        def rest():
            for r in range(min(bits, chunks), bits):
                step(r)
            finish()

        return start, after, rest

    start, after, rest = scan_ops(0, states.at[chunks], s0)
    start()

    def rows_of(c):
        return pl.ds(pl.multiple_of(c * Q, Q), Q)

    def intra_forward(c, carry):
        rows = rows_of(c)
        in_low = act[rows, pl.ds(DI, NSTATE)].astype(bf16)
        out_low = act[rows, pl.ds(DI + NSTATE, NSTATE)].astype(bf16)
        scores = mm_nt(out_low, in_low) * lower_f
        for p in range(PAIRS):
            parts = []
            for h in (2 * p, 2 * p + 1):
                spread = cum[rows, h : h + 1] - cum_t[c, h : h + 1, :]
                parts.append((scores * jnp.exp(jnp.minimum(spread, 0.0))).astype(bf16))
            stepped = (act[rows, pair(p)] * ex_dt[rows, pair(p)].astype(f32)).astype(bf16)
            yst[rows, pair(p)] = mm(jnp.concatenate(parts, axis=1), blockdiag(stepped))
        after(c)
        return carry

    lax.fori_loop(0, chunks, intra_forward, 0)
    rest()

    sum_conv[...] = jnp.zeros_like(sum_conv)
    sum_gate[...] = jnp.zeros_like(sum_gate)
    gain_wide = gain[0:1, :]

    def state_decay(c):
        last = jnp.broadcast_to(cum_t[c][:, Q - 1 : Q], (NHEADS, 8))
        wide = jnp.concatenate([last, jnp.zeros((LANES - NHEADS, 8), f32)], axis=0)
        return wide.T[:, 0:NHEADS]

    def gating(c, before):
        rows = rows_of(c)
        decay_before = widen(jnp.exp(before), spread_m)
        out_now = act[rows, pl.ds(DI + NSTATE, NSTATE)]
        out_low = out_now.astype(bf16)
        out_t = out_now.T.astype(bf16)
        squares = jnp.zeros((Q, LANES), f32)
        for p in range(PAIRS):
            state = states[c, :, pair(p)] + decay_before[:, p * LANES : (p + 1) * LANES] * s0[
                :, pair(p)
            ]
            states[c, :, pair(p)] = state
            reached = ex_e[rows, pair(p)].astype(f32) * mm(out_low, state.astype(bf16))
            with_skip = (
                yst[rows, pair(p)]
                + reached
                + skip_wide[:, p * LANES : (p + 1) * LANES] * act[rows, pair(p)]
            )
            z = proj[rows, pair(p)].astype(f32)
            sig = sigmoid(z)
            gated = with_skip * (z * sig)
            squares += gated * gated
            yint[:, pair(p)] = reached
            ws[:, pair(p)] = with_skip
            sg[:, pair(p)] = sig
        norm = lax.rsqrt(jnp.sum(squares, axis=1, keepdims=True) * (1.0 / DI) + epsilon)
        inner = jnp.zeros((Q, LANES), f32)
        for p in range(PAIRS):
            z = proj[rows, pair(p)].astype(f32)
            gated = ws[:, pair(p)] * (z * sg[:, pair(p)])
            gain_p = gain_wide[:, p * LANES : (p + 1) * LANES]
            gate_low[rows, pair(p)] = (gated * norm * gain_p).astype(bf16)
            inner += grad_low[rows, pair(p)] * gain_p * gated
            sum_gate[0:8, pair(p)] += fold_rows(grad_low[rows, pair(p)] * (gated * norm))
        mean = jnp.sum(inner, axis=1, keepdims=True) * (1.0 / DI)
        pull = norm * norm * norm * mean
        later = jnp.zeros((Q, NHEADS), f32)
        for p in range(PAIRS):
            z = proj[rows, pair(p)].astype(f32)
            sig = sg[:, pair(p)]
            with_skip = ws[:, pair(p)]
            gain_p = gain_wide[:, p * LANES : (p + 1) * LANES]
            gated = with_skip * (z * sig)
            grad_gated = norm * (grad_low[rows, pair(p)] * gain_p) - gated * pull
            grad = grad_gated * (z * sig)
            gs[rows, pair(p)] = grad
            grad_z = grad_gated * with_skip * (sig * (1.0 + z * (1.0 - sig)))
            grad_proj[rows, pair(p)] = grad_z.astype(bf16)
            sum_gate[8:16, pair(p)] += fold_rows(grad * act[rows, pair(p)])
            later += mm((grad * yint[:, pair(p)]).astype(bf16), gather_m(p))
            scaled = (grad * ex_e[rows, pair(p)].astype(f32)).astype(bf16)
            adjs[c, :, pair(p)] = mm(out_t, scaled)
        grad_a[rows, :] = mm_exact(upper_f, later)
        return before + state_decay(c)

    lax.fori_loop(0, chunks, gating, jnp.zeros((8, NHEADS), f32))

    adjs[chunks] = jnp.zeros((NSTATE, DI), f32)

    def local_adjoints(i, carry):
        c = chunks - 1 - i
        decay = widen(jnp.exp(state_decay(c)), spread_m)
        for p in range(PAIRS):
            adjs[c, :, pair(p)] = (
                decay[:, p * LANES : (p + 1) * LANES] * adjs[c + 1, :, pair(p)]
                + adjs[c, :, pair(p)]
            )
        return carry

    lax.fori_loop(0, chunks, local_adjoints, 0)
    start, after, rest = scan_ops(1, adjs.at[0], g0)
    start()

    def intra_backward(c, carry):
        rows = rows_of(c)
        in_low = act[rows, pl.ds(DI, NSTATE)].astype(bf16)
        out_low = act[rows, pl.ds(DI + NSTATE, NSTATE)].astype(bf16)
        scores = mm_nt(in_low, out_low) * upper_f
        grad_scores = jnp.zeros((Q, Q), f32)
        tails = upper_f.T.astype(bf16)
        found = []
        for p in range(PAIRS):
            grad = gs[rows, pair(p)].astype(bf16)
            stepped = (act[rows, pair(p)] * ex_dt[rows, pair(p)].astype(f32)).astype(bf16)
            values = mm_nt(blockdiag(stepped), grad)
            weights, crosses = [], []
            for i, h in enumerate((2 * p, 2 * p + 1)):
                spread = cum_t[c, h : h + 1, :] - cum[rows, h : h + 1]
                decays = jnp.exp(jnp.minimum(spread, 0.0))
                weights.append((scores * decays).astype(bf16))
                part = decays * values[i * Q : (i + 1) * Q, :]
                grad_scores += part
                crosses.append((part * scores).astype(bf16))
            yst[rows, pair(p)] = mm(jnp.concatenate(weights, axis=1), blockdiag(grad))
            sums = mm(jnp.concatenate(crosses, axis=0), tails)
            for i in range(2):
                picked = jnp.where(strict_upper, sums[i * Q : (i + 1) * Q, :], 0.0)
                found.append(jnp.sum(picked, axis=0, keepdims=True))
        found.append(jnp.zeros((LANES - NHEADS, Q), f32))
        grad_a[rows, :] += jnp.concatenate(found, axis=0).T[:, 0:NHEADS]
        grad_low_scores = (grad_scores * upper_f).astype(bf16)
        gpad[rows, pl.ds(DI, NSTATE)] = mm(grad_low_scores, out_low)
        gpad[rows, pl.ds(DI + NSTATE, NSTATE)] = mm((grad_scores * upper_f).T.astype(bf16), in_low)
        after(c)
        return carry

    lax.fori_loop(0, chunks, intra_backward, 0)
    rest()

    sum_head[...] = jnp.zeros_like(sum_head)

    def finish_backward(c, before):
        after_log = jnp.broadcast_to(log_total, (8, NHEADS)) - before - state_decay(c)
        decay_after = widen(jnp.exp(after_log), spread_m)
        rows = rows_of(c)
        in_low = act[rows, pl.ds(DI, NSTATE)].astype(bf16)
        grad_in = gpad[rows, pl.ds(DI, NSTATE)]
        grad_out = gpad[rows, pl.ds(DI + NSTATE, NSTATE)]
        kept = jnp.zeros((Q, NHEADS), f32)
        grad_step = jnp.zeros((Q, NHEADS), f32)
        crossing = jnp.zeros((8, NHEADS), f32)
        for p in range(PAIRS):
            adj = adjs[c + 1, :, pair(p)] + decay_after[:, p * LANES : (p + 1) * LANES] * g0[
                :, pair(p)
            ]
            adj_low = adj.astype(bf16)
            state = states[c, :, pair(p)]
            x = act[rows, pair(p)]
            dt = ex_dt[rows, pair(p)].astype(f32)
            to_end = ex_f[rows, pair(p)].astype(f32)
            grad = gs[rows, pair(p)]
            later = to_end * mm(in_low, adj_low)
            total = yst[rows, pair(p)] + later
            stepped = x * dt
            pick = gather_m(p)
            kept += mm((stepped * later).astype(bf16), pick)
            grad_step += mm((x * total).astype(bf16), pick)
            crossing += mm(fold_rows(adj * state).astype(bf16), pick)
            grad_in += mm_nt((stepped * to_end).astype(bf16), adj_low)
            scaled = (grad * ex_e[rows, pair(p)].astype(f32)).astype(bf16)
            grad_out += mm_nt(scaled, state.astype(bf16))
            grad_x = dt * total + skip_wide[:, p * LANES : (p + 1) * LANES] * grad
            gpad[rows, pair(p)] = grad_x * dsilu[rows, pair(p)]
        gpad[rows, pl.ds(DI, NSTATE)] = grad_in * dsilu[rows, pl.ds(DI, NSTATE)]
        gpad[rows, pl.ds(DI + NSTATE, NSTATE)] = grad_out * dsilu[rows, pl.ds(DI + NSTATE, NSTATE)]
        whole = jnp.exp(state_decay(c))[0:1, :] * jnp.sum(crossing, axis=0, keepdims=True)
        grad_decay = grad_a[rows, :] + mm_exact(lower_f - upper_f * lower_f, kept) + whole
        grad_raw = (grad_step - rate * grad_decay) * sgm[rows, :]
        grad_proj[rows, pl.ds(DI + DC, NHEADS)] = grad_raw.astype(bf16)
        sum_head[0:8, 0:NHEADS] += fold_rows(grad_raw)
        sum_head[8:16, 0:NHEADS] += fold_rows(grad_decay * logd[rows, :])

        @pl.when(jnp.logical_and(c == 0, me > 0))
        def _():
            grad_edge_copy().start()

        return before + state_decay(c)

    lax.fori_loop(0, chunks, finish_backward, jnp.zeros((8, NHEADS), f32))

    @pl.when(me > 0)
    def _():
        grad_edge_copy().wait_send()

    @pl.when(me < seq_size - 1)
    def _():
        grad_edge_copy().wait_recv()
        gpad[pl.ds(length, 8), :] = grad_edge[...]

    @pl.when(me == seq_size - 1)
    def _():
        gpad[pl.ds(length, 8), :] = jnp.zeros((8, DC), f32)

    def conv_backward(c, carry):
        rows = rows_of(c)
        longer = pl.ds(pl.multiple_of(c * Q, Q), Q + 8)
        for block in range(DC // LANES):
            lanes = pl.ds(block * LANES, LANES)
            grads = gpad[longer, lanes]
            inputs = cpad[longer, lanes]
            grad = grads[0:Q, :]
            grad_conv = sum(
                taps[k : k + 1, lanes] * grads[KCONV - 1 - k : KCONV - 1 - k + Q, :]
                for k in range(KCONV)
            )
            grad_proj[rows, pl.ds(DI + block * LANES, LANES)] = grad_conv.astype(bf16)
            for k in range(KCONV):
                sum_conv[8 * k : 8 * k + 8, lanes] += fold_rows(grad * inputs[5 + k : 5 + k + Q, :])
            sum_conv[8 * KCONV : 8 * KCONV + 8, lanes] += fold_rows(grad)
        return carry

    lax.fori_loop(0, chunks, conv_backward, 0)


def ssd_call(seq_size, proj, grad_low, taps, cbias, heads, gain):
    length = proj.shape[0]
    chunks = length // Q
    bits = seq_size.bit_length() - 1
    vmem = lambda shape, kind=f32: pltpu.VMEM(shape, kind)
    space = pl.BlockSpec(memory_space=pltpu.VMEM)
    return pl.pallas_call(
        functools.partial(ssd_kernel, seq_size),
        name="ssd",
        out_shape=(
            jax.ShapeDtypeStruct((length, DI), bf16),
            jax.ShapeDtypeStruct((length, proj.shape[1]), bf16),
            jax.ShapeDtypeStruct((8 * (KCONV + 1), DC), f32),
            jax.ShapeDtypeStruct((16, DI), f32),
            jax.ShapeDtypeStruct((16, LANES), f32),
        ),
        in_specs=[space] * 6,
        out_specs=[space] * 5,
        scratch_shapes=[
            vmem((length + 8, DC)),
            vmem((length, DC)),
            vmem((length, DC)),
            vmem((length + 8, DC)),
            vmem((Q, DI)),
            vmem((length, DI)),
            vmem((Q, DI)),
            vmem((Q, DI)),
            vmem((length, DI)),
            vmem((length, DI), bf16),
            vmem((length, DI), bf16),
            vmem((length, DI), bf16),
            vmem((length, NHEADS)),
            vmem((chunks, NHEADS, Q)),
            vmem((length, NHEADS)),
            vmem((length, NHEADS)),
            vmem((length, NHEADS)),
            vmem((length, NHEADS)),
            vmem((chunks + 1, NSTATE, DI)),
            vmem((chunks + 1, NSTATE, DI)),
            vmem((NSTATE, DI)),
            vmem((NSTATE, DI)),
            vmem((16, DC), bf16),
            vmem((8, DC)),
            vmem((2, 2, NSTATE, HALF), bf16),
            vmem((2, 2, NSTATE, HALF), bf16),
            vmem((2 * bits, NSTATE, HALF), bf16),
            vmem((2 * bits, NSTATE, HALF), bf16),
            vmem((2, NSTATE, HALF), bf16),
            vmem((2, NSTATE, HALF), bf16),
            vmem((bits, 8, LANES)),
            vmem((bits, 8, LANES)),
            pltpu.SemaphoreType.DMA((4,)),
            pltpu.SemaphoreType.DMA((2, 2)),
            pltpu.SemaphoreType.DMA((2 * bits, 2)),
            pltpu.SemaphoreType.DMA((2, 2)),
            pltpu.SemaphoreType.DMA((bits, 2)),
            vmem((2, NSTATE, HALF)),
            vmem((2, 8, NHEADS)),
        ],
        compiler_params=pltpu.CompilerParams(
            collective_id=1, has_side_effects=True, vmem_limit_bytes=62 * 1024 * 1024
        ),
    )(proj, grad_low, taps, cbias, heads, gain)


def mesh_digits(sizes):
    steps = [("seq", 1 << r, 2) for r in range(sizes["seq"].bit_length() - 1)]
    first = [("dp", 1, sizes["dp"])]
    return first + steps[1:] + steps[:1], first + steps[:0:-1] + steps[:1]


def digit_of(digit):
    axis, stride, size = digit
    return (lax.axis_index(axis) // stride) % size


def moved(digit, offset):
    axis, stride, size = digit
    now = digit_of(digit)
    return lax.axis_index(axis) + ((now + offset) % size - now) * stride


def rank_at(sizes, changes):
    place = {axis: lax.axis_index(axis) for axis in sizes}
    for digit, offset in changes:
        axis, stride, size = digit
        now = digit_of(digit)
        place[axis] = place[axis] + ((now + offset) % size - now) * stride
    return place["dp"] * sizes["seq"] + place["seq"]


def greet(sizes):
    barrier = pltpu.get_barrier_semaphore()
    count = 0
    for digit in mesh_digits(sizes)[0]:
        for offset in range(1, digit[2]):
            pl.semaphore_signal(
                barrier, inc=1, device_id={digit[0]: moved(digit, offset)}, device_id_type=MESH
            )
            count += 1
    pl.semaphore_wait(barrier, count)


def spans(width, parts):
    tiles = width // LANES
    edges = [tiles * k // parts * LANES for k in range(parts)] + [width]
    return [(edges[k], edges[k + 1] - edges[k]) for k in range(parts)]


def gather_kernel(sizes, *refs):
    items = 3
    sources, targets = refs[:items], refs[items : 2 * items]
    own_sems, sends, arrivals = refs[2 * items :]
    greet(sizes)
    orders = mesh_digits(sizes)
    mine = rank_at(sizes, [])
    for k in range(items):
        pltpu.make_async_copy(sources[k], targets[k].at[mine], own_sems.at[k]).start()

    streams = []
    for k in range(items):
        width = sources[k].shape[1]
        for j, (at, size) in enumerate(spans(width, 2 if width > 512 else 1)):
            streams.append((k, at, size, orders[j], len(streams)))
    used = [0] * len(streams)
    waits = []

    def copy(stream, changes, digit, offset, first):
        k, at, size, _, index = stream
        slot = rank_at(sizes, changes)
        lanes = pl.ds(at, size)
        source = sources[k].at[:, lanes] if first else targets[k].at[slot, :, lanes]
        return pltpu.make_async_remote_copy(
            src_ref=source,
            dst_ref=targets[k].at[slot, :, lanes],
            send_sem=sends.at[index, used[index]],
            recv_sem=arrivals.at[index, slot],
            device_id={digit[0]: moved(digit, offset)},
            device_id_type=MESH,
        )

    def pass_on(stream, changes, depth):
        order = stream[3]
        for position in range(depth, len(order)):
            digit = order[position]
            for offset in range(1, digit[2]):
                started = copy(stream, changes, digit, offset, not changes)
                used[stream[4]] += 1
                started.start()
                waits.append(started)

    def arrived(stream, changes):
        k, at, size, _, index = stream
        slot = rank_at(sizes, changes)
        lanes = pl.ds(at, size)
        pltpu.make_async_remote_copy(
            src_ref=targets[k].at[slot, :, lanes],
            dst_ref=targets[k].at[slot, :, lanes],
            send_sem=sends.at[index, 0],
            recv_sem=arrivals.at[index, slot],
            device_id={"dp": moved(orders[0][0], 1)},
            device_id_type=MESH,
        ).wait_recv()

    def shards(order, depth):
        found = [[]]
        for position in range(depth):
            found = [
                held + ([(order[position], offset)] if offset else [])
                for held in found
                for offset in range(order[position][2])
            ]
        return [
            held + [(order[depth], offset)] for held in found for offset in range(1, order[depth][2])
        ]

    for stream in streams:
        pass_on(stream, [], 0)
    for depth in range(len(orders[0])):
        lists = [(stream, shards(stream[3], depth)) for stream in streams]
        for turn in range(len(lists[0][1])):
            for stream, held in lists:
                arrived(stream, held[turn])
                pass_on(stream, held[turn], depth + 1)
    for started in waits:
        started.wait_send()
    for k in range(items):
        pltpu.make_async_copy(sources[k], targets[k].at[mine], own_sems.at[k]).wait()


def gather_call(sizes, *arrays):
    count = sizes["dp"] * sizes["seq"]
    streams = 5
    return pl.pallas_call(
        functools.partial(gather_kernel, sizes),
        name="gather",
        out_shape=tuple(jax.ShapeDtypeStruct((count,) + a.shape, a.dtype) for a in arrays),
        in_specs=[pl.BlockSpec(memory_space=pltpu.VMEM)] * len(arrays),
        out_specs=[pl.BlockSpec(memory_space=pl.ANY)] * len(arrays),
        scratch_shapes=[
            pltpu.SemaphoreType.DMA((len(arrays),)),
            pltpu.SemaphoreType.DMA((streams, count)),
            pltpu.SemaphoreType.DMA((streams, count)),
        ],
        compiler_params=pltpu.CompilerParams(collective_id=2, has_side_effects=True),
    )(*arrays)


def scatter_kernel(sizes, parts, items, *refs):
    orders = mesh_digits(sizes)
    depth = len(orders[0])
    lengths = [digit[2] for digit in orders[0]]
    counts = [1]
    for size in lengths:
        counts.append(counts[-1] * size)
    sources, refs = refs[:items], refs[items:]
    targets, refs = refs[:items], refs[items:]
    sums, refs = refs[:items], refs[items:]
    landed, refs = refs[: items * depth], refs[items * depth :]
    sends, arrivals = refs
    greet(sizes)

    streams = []
    for k in range(items):
        for j, (at, size) in enumerate(spans(sources[k].shape[2], parts[k])):
            streams.append((k, pl.ds(at, size), orders[j % 2], len(streams)))
    base = [0]
    for position in range(depth):
        base.append(base[-1] + (lengths[position] - 1) * counts[position])
    started, waiting = [], []

    def offsets_of(relative):
        found = []
        for size in lengths:
            found.append(relative % size)
            relative //= size
        return found

    def copy(stream, position, offset, relative):
        k, lanes, order, index = stream
        digit = order[position]
        if position == depth - 1:
            changes = list(zip(order, offsets_of(relative) [:position] + [offset]))
            source = sources[k].at[rank_at(sizes, changes), :, lanes]
        else:
            source = sums[k].at[offset * counts[position] + relative, :, lanes]
        there = (digit[2] - offset - 1) * counts[position] + relative
        return pltpu.make_async_remote_copy(
            src_ref=source,
            dst_ref=landed[k * depth + position].at[there, :, lanes],
            send_sem=sends.at[index, base[position] + there],
            recv_sem=arrivals.at[index, base[position] + there],
            device_id={digit[0]: moved(digit, offset)},
            device_id_type=MESH,
        )

    def flush(keep):
        while len(waiting) > keep:
            item = waiting.pop(0)
            item.start()
            started.append(item)

    def receive(stream, position, relative):
        k, lanes, order, index = stream
        if position == depth - 1:
            own = list(zip(order, offsets_of(relative)[:position]))
            total = sources[k][rank_at(sizes, own), :, lanes].astype(f32)
        else:
            total = sums[k][relative, :, lanes].astype(f32)
        buffer = landed[k * depth + position]
        for offset in range(1, lengths[position]):
            here = (offset - 1) * counts[position] + relative
            pltpu.make_async_remote_copy(
                src_ref=buffer.at[here, :, lanes],
                dst_ref=buffer.at[here, :, lanes],
                send_sem=sends.at[index, base[position] + here],
                recv_sem=arrivals.at[index, base[position] + here],
                device_id={order[position][0]: moved(order[position], offset)},
                device_id_type=MESH,
            ).wait_recv()
            total += buffer[here, :, lanes].astype(f32)
        if position == 0:
            targets[k][:, lanes] = total
            return
        sums[k][relative, :, lanes] = total.astype(sums[k].dtype)
        offset, below = divmod(relative, counts[position - 1])
        if offset:
            waiting.append(copy(stream, position - 1, offset, below))

    for relative in reversed(range(counts[depth - 1])):
        for stream in streams:
            for offset in range(1, lengths[depth - 1]):
                waiting.append(copy(stream, depth - 1, offset, relative))
                flush(0)
    for position in reversed(range(depth)):
        for relative in reversed(range(counts[position])):
            for stream in streams:
                receive(stream, position, relative)
                flush(1)
        flush(0)
    for item in started:
        item.wait_send()


def scatter_call(sizes, parts, *arrays):
    depth = sizes["seq"].bit_length()
    lengths = [sizes["dp"]] + [2] * (depth - 1)
    counts = [1]
    for size in lengths:
        counts.append(counts[-1] * size)
    most = sum((lengths[j] - 1) * counts[j] for j in range(depth))
    scratch = [pltpu.VMEM((counts[depth - 1],) + a.shape[1:], a.dtype) for a in arrays]
    for a in arrays:
        for j in range(depth):
            scratch.append(pltpu.VMEM(((lengths[j] - 1) * counts[j],) + a.shape[1:], a.dtype))
    return pl.pallas_call(
        functools.partial(scatter_kernel, sizes, parts, len(arrays)),
        name="scatter",
        out_shape=tuple(jax.ShapeDtypeStruct(a.shape[1:], f32) for a in arrays),
        in_specs=[pl.BlockSpec(memory_space=pltpu.VMEM)] * len(arrays),
        out_specs=[pl.BlockSpec(memory_space=pltpu.VMEM)] * len(arrays),
        scratch_shapes=scratch
        + [
            pltpu.SemaphoreType.DMA((sum(parts), most)),
            pltpu.SemaphoreType.DMA((sum(parts), most)),
        ],
        compiler_params=pltpu.CompilerParams(
            collective_id=3, has_side_effects=True, vmem_limit_bytes=62 * 1024 * 1024
        ),
    )(*arrays)


class Place:
    def __init__(self):
        self.z = lax.axis_index("dp")
        seq = lax.axis_index("seq")
        self.seq = seq
        self.y = seq // 4
        self.x = (seq // 2) % 2
        self.c = seq % 2
        self.over_x = {"seq": seq + 2 - 4 * self.x}
        self.over_y = {"seq": seq + 4 - 8 * self.y}
        self.sibling = {"seq": seq + 1 - 2 * self.c}
        near = self.z < 2
        self.mate = self.z + 1 - 2 * (self.z % 2)
        self.planes = [self.z, self.mate, jnp.where(near, 2, 1), jnp.where(near, 3, 0)]
        self.inner = jnp.logical_or(self.z == 1, self.z == 2)
        self.across = 3 - self.z

    def slot(self, o=0, y=0, x=0, c=0):
        across = self.seq
        across = across + (4 - 8 * self.y if y else 0)
        across = across + (2 - 4 * self.x if x else 0)
        across = across + (1 - 2 * self.c if c else 0)
        return self.planes[o] * 8 + across

    def greet(self):
        barrier = pltpu.get_barrier_semaphore()
        for other in (self.over_x, self.over_y, self.sibling):
            pl.semaphore_signal(barrier, inc=1, device_id=other, device_id_type=MESH)
        for o in range(1, 4):
            pl.semaphore_signal(
                barrier, inc=1, device_id={"dp": self.planes[o]}, device_id_type=MESH
            )
        pl.semaphore_wait(barrier, 6)


def remote(source, target, send, arrival, device):
    return pltpu.make_async_remote_copy(
        src_ref=source,
        dst_ref=target,
        send_sem=send,
        recv_sem=arrival,
        device_id=device,
        device_id_type=MESH,
    )


class Gather:
    SENDS = 37

    def __init__(self, place, source, target, sends, arrivals, cut):
        self.place = place
        self.source = source
        self.target = target
        self.sends = sends
        self.arrivals = arrivals
        width = source.shape[-1]
        self.halves = (pl.ds(0, cut), pl.ds(cut, width - cut)) if cut else (pl.ds(0, width),) * 2
        self.split = cut > 0
        self.started = []

    def send(self, slot, device, half=None, own=False, when=None):
        at = self.target(slot)
        start = self.source if own else at
        part = 0
        if half is not None:
            if not self.split and half == 1:
                return
            part = half
            start, at = start.at[:, self.halves[half]], at.at[:, self.halves[half]]
        k = len(self.started)
        copy = remote(start, at, self.sends.at[k], self.arrivals.at[slot, part], device)
        if when is None:
            copy.start()
        else:
            pl.when(when)(copy.start)
        self.started.append((copy, when))

    def wait(self, slot, half=None):
        at = self.target(slot)
        part = 0
        if half is not None:
            if not self.split and half == 1:
                return
            part = half
            at = at.at[:, self.halves[half]]
        remote(at, at, self.sends.at[0], self.arrivals.at[slot, part], self.place.sibling).wait_recv()

    def spread(self, o, own=False):
        place = self.place
        slot = place.slot(o)
        self.send(slot, place.over_x, own=own)
        self.send(slot, place.over_y, own=own)
        self.send(slot, place.sibling, own=own)

    def start(self):
        self.send(self.place.slot(), {"dp": self.place.mate}, own=True)
        self.inward(0, self.place.across, own=True)
        self.spread(0, own=True)

    def inward(self, o, plane, own=False):
        place = self.place
        self.send(place.slot(o), {"dp": plane}, own=own, when=place.inner)

    def steps(self):
        place = self.place

        def plane(o):
            self.wait(place.slot(o))
            self.inward(o, place.across if o == 1 else place.mate)
            self.spread(o)

        def side(o):
            slot = place.slot(o, x=1)
            self.wait(slot)
            self.send(slot, place.over_y, half=0)
            self.send(slot, place.sibling)
            slot = place.slot(o, y=1)
            self.wait(slot)
            self.send(slot, place.over_x, half=1)
            self.send(slot, place.sibling)

        def corner(o):
            slot = place.slot(o, x=1, y=1)
            self.wait(slot, half=0)
            self.wait(slot, half=1)
            self.send(slot, place.sibling)

        order = [(plane, 1), (side, 0), (plane, 2), (corner, 0), (side, 1), (plane, 3), (corner, 1)]
        order += [(side, 2), (corner, 2), (side, 3), (corner, 3)]
        return [functools.partial(step, o) for step, o in order] + [self.core]

    def core(self):
        for o in range(4):
            for y in range(2):
                for x in range(2):
                    self.wait(self.place.slot(o, y, x, 1))

    def drain(self):
        for copy, when in self.started:
            if when is None:
                copy.wait_send()
            else:
                pl.when(when)(copy.wait_send)


def quick_gather_kernel(*refs):
    items = 3
    sources, targets = refs[:items], refs[items : 2 * items]
    own_sems = refs[2 * items]
    sems = refs[2 * items + 1 :]
    place = Place()
    place.greet()
    gathers = []
    for k in range(items):
        width = sources[k].shape[1]
        cut = width // (2 * LANES) * LANES if width > 512 else 0
        gathers.append(
            Gather(place, sources[k], targets[k].at.__getitem__, sems[2 * k], sems[2 * k + 1], cut)
        )
    mine = place.slot()
    for k in range(items):
        pltpu.make_async_copy(sources[k], targets[k].at[mine], own_sems.at[k]).start()
        gathers[k].start()
    for steps in zip(*(gather.steps() for gather in gathers)):
        for step in steps:
            step()
    for k in range(items):
        gathers[k].drain()
        pltpu.make_async_copy(sources[k], targets[k].at[mine], own_sems.at[k]).wait()


def quick_gather_call(*arrays):
    count = 32
    sems = []
    for _ in arrays:
        sems += [pltpu.SemaphoreType.DMA((Gather.SENDS,)), pltpu.SemaphoreType.DMA((count, 2))]
    return pl.pallas_call(
        quick_gather_kernel,
        name="gather",
        out_shape=tuple(jax.ShapeDtypeStruct((count,) + a.shape, a.dtype) for a in arrays),
        in_specs=[pl.BlockSpec(memory_space=pltpu.VMEM)] * len(arrays),
        out_specs=[pl.BlockSpec(memory_space=pl.ANY)] * len(arrays),
        scratch_shapes=[pltpu.SemaphoreType.DMA((len(arrays),))] + sems,
        compiler_params=pltpu.CompilerParams(collective_id=5, has_side_effects=True),
    )(*arrays)


class Reduce:
    def __init__(self, place, refs, cut):
        self.place = place
        (self.part, self.sums, self.land_c, self.land_x, self.land_y, self.land_xy, self.land_z) = refs[:7]
        (self.sems_c, self.sems_a, self.sems_b, self.sems_z) = refs[7:]
        width = self.part.shape[-1]
        self.halves = (pl.ds(0, cut), pl.ds(cut, width - cut))

    @staticmethod
    def scratch(rows, width, cut, kind):
        vmem = lambda *shape: pltpu.VMEM(shape + (rows, width), kind)
        half = lambda size: pltpu.VMEM((4, 2, rows, size), kind)
        dma = pltpu.SemaphoreType.DMA
        return [
            vmem(4, 2, 2, 2),
            vmem(4, 2, 2),
            vmem(4, 2, 2),
            half(cut),
            half(width - cut),
            vmem(4),
            vmem(4),
            dma((4, 2)),
            dma((4, 2, 2)),
            dma((4, 2, 2)),
            dma((4, 2)),
        ]

    def copy_c(self, o):
        z, place = self.place.planes[o], self.place
        return remote(
            self.part.at[z, :, :, 1 - place.c],
            self.land_c.at[z],
            self.sems_c.at[z, 0],
            self.sems_c.at[z, 1],
            place.sibling,
        )

    def copy_first(self, o, half):
        z, place = self.place.planes[o], self.place
        lanes = self.halves[half]
        if half == 0:
            source, target = self.sums.at[z, :, 1 - place.x, :, lanes], self.land_x.at[z]
        else:
            source, target = self.sums.at[z, 1 - place.y, :, :, lanes], self.land_y.at[z]
        device = place.over_y if half else place.over_x
        return remote(source, target, self.sems_a.at[z, half, 0], self.sems_a.at[z, half, 1], device)

    def copy_second(self, o, half):
        z, place = self.place.planes[o], self.place
        lanes = self.halves[half]
        y, x = (place.y, 1 - place.x) if half else (1 - place.y, place.x)
        device = place.over_x if half else place.over_y
        return remote(
            self.sums.at[z, y, x, :, lanes],
            self.land_xy.at[z, :, lanes],
            self.sems_b.at[z, half, 0],
            self.sems_b.at[z, half, 1],
            device,
        )

    def copy_plane(self, o):
        place = self.place
        z = place.planes[o]
        return remote(
            self.sums.at[z, place.y, place.x],
            self.land_z.at[place.z],
            self.sems_z.at[z, 0],
            self.sems_z.at[place.z, 1],
            {"dp": z},
        )

    def give(self, o):
        self.copy_c(o).start()

    def cores(self, o):
        place, z = self.place, self.place.planes[o]
        self.copy_c(o).wait_recv()
        for y in range(2):
            for x in range(2):
                own = self.part[z, y, x, place.c].astype(f32)
                self.sums[z, y, x] = (own + self.land_c[z, y, x].astype(f32)).astype(self.sums.dtype)
        self.copy_first(o, 0).start()
        self.copy_first(o, 1).start()

    def firsts(self, o):
        place, z = self.place, self.place.planes[o]
        for half in range(2):
            lanes = self.halves[half]
            self.copy_first(o, half).wait_recv()
            landed = self.land_y if half else self.land_x
            for k in range(2):
                y, x = (place.y, k) if half else (k, place.x)
                own = self.sums[z, y, x, :, lanes].astype(f32)
                self.sums[z, y, x, :, lanes] = (own + landed[z, k].astype(f32)).astype(
                    self.sums.dtype
                )
            self.copy_second(o, half).start()

    def seconds(self, o):
        place, z = self.place, self.place.planes[o]
        self.copy_second(o, 0).wait_recv()
        self.copy_second(o, 1).wait_recv()
        own = self.sums[z, place.y, place.x].astype(f32)
        total = own + self.land_xy[z].astype(f32)
        if o == 0:
            return total
        self.sums[z, place.y, place.x] = total.astype(self.sums.dtype)
        self.copy_plane(o).start()

    def last(self, total, target):
        for o in range(1, 4):
            z = self.place.planes[o]
            remote(
                self.land_z.at[z],
                self.land_z.at[z],
                self.sems_z.at[z, 0],
                self.sems_z.at[z, 1],
                {"dp": z},
            ).wait_recv()
            total += self.land_z[z].astype(f32)
        target[...] = total

    def drain(self):
        for o in range(4):
            self.copy_c(o).wait_send()
            for half in range(2):
                self.copy_first(o, half).wait_send()
                self.copy_second(o, half).wait_send()
            if o:
                self.copy_plane(o).wait_send()


FIELDS = KCONV + 6


def finish_kernel(rows_in, rows_out, *refs):
    (tokens, cotangent, norm_gain, grad_proj, gate_low, in_full, out_full) = refs[:7]
    (sum_conv, sum_gate, sum_head) = refs[7:10]
    (block_out, input_grad, inward, outward) = refs[10:14]
    (norm_grad, kernel_grad, offset_grad, gain_grad, step_grad, decay_grad, skip_grad) = refs[14:21]
    refs = refs[21:]
    (normed_t, small_out, norm_sum) = refs[:3]
    refs = refs[3:]
    place = Place()
    cuts = (grad_proj.shape[1] // (2 * LANES) * LANES, tokens.shape[1] // 2, FIELDS * LANES // 2)
    reduce_in, reduce_out, reduce_small = [
        Reduce(place, refs[11 * k : 11 * k + 11], cuts[k]) for k in range(3)
    ]
    length = tokens.shape[0]
    width = tokens.shape[1]
    columns = grad_proj.shape[1]
    count = 32
    place.greet()

    gain = norm_gain[...]

    def normalize(c, carry):
        rows = pl.ds(pl.multiple_of(c * Q, Q), Q)
        values = tokens[rows, :].astype(f32)
        scale = lax.rsqrt(jnp.sum(values * values, axis=1, keepdims=True) * (1.0 / width) + epsilon)
        normed_t[c] = (values * scale * gain).T.astype(bf16)
        return carry

    lax.fori_loop(0, length // Q, normalize, 0)

    def multiply_in(o):
        plane = place.planes[o]
        at = pl.multiple_of(plane * (8 * rows_in), 64)
        left = jnp.concatenate(
            [normed_t[c, pl.ds(at, 8 * rows_in), :] for c in range(length // Q)], axis=1
        )
        for lane in range(0, columns, 512):
            size = min(512, columns - lane)
            block = mm(left, grad_proj[:, pl.ds(lane, size)])
            for k in range(8):
                reduce_in.part[plane, k // 4, (k // 2) % 2, k % 2, :, pl.ds(lane, size)] = block[
                    k * rows_in : (k + 1) * rows_in, :
                ].astype(bf16)
        reduce_in.give(o)

    def multiply_out(o):
        plane = place.planes[o]
        at = pl.multiple_of(plane * (8 * rows_out), LANES)
        left = gate_low[:, pl.ds(at, 8 * rows_out)].astype(f32).T.astype(bf16)
        block = mm(left, cotangent[...])
        for k in range(8):
            reduce_out.part[plane, k // 4, (k // 2) % 2, k % 2] = block[
                k * rows_out : (k + 1) * rows_out, :
            ].astype(bf16)
        reduce_out.give(o)

    norm_sum[...] = jnp.zeros_like(norm_sum)

    def inputs_of(c):
        rows = pl.ds(pl.multiple_of(c * Q, Q), Q)
        values = tokens[rows, :].astype(f32)
        grad_normed = mm_nt(grad_proj[rows, :], in_full[...])
        scale = lax.rsqrt(jnp.sum(values * values, axis=1, keepdims=True) * (1.0 / width) + epsilon)
        norm_sum[...] += fold_rows(grad_normed * (values * scale))
        weighted = grad_normed * gain
        mean = jnp.sum(weighted * values, axis=1, keepdims=True) * (1.0 / width)
        back = scale * weighted - values * (scale * scale * scale * mean)
        input_grad[rows, :] = (back + cotangent[rows, :].astype(f32)).astype(bf16)
        block_out[rows, :] = (values + mm(gate_low[rows, :], out_full[...])).astype(bf16)


    def total_of(ref, k):
        return jnp.sum(ref[8 * k : 8 * k + 8, :], axis=0, keepdims=True)

    part_small = reduce_small.part

    def spread_slots(row, field, per):
        for r in range(count):
            part_small[r // 8, (r // 4) % 2, (r // 2) % 2, r % 2, :, pl.ds(field * LANES, per)] = row[:, r * per : (r + 1) * per]

    def small_parts():

        part_small[...] = jnp.zeros_like(part_small)
        spread_slots(total_of(norm_sum, 0), 0, width // count)
        for k in range(KCONV + 1):
            spread_slots(total_of(sum_conv, k), 1 + k, DC // count)
        spread_slots(total_of(sum_gate, 0), 2 + KCONV, DI // count)
        skip_row = jnp.broadcast_to(total_of(sum_gate, 1), (8, DI))
        lane_head = lax.broadcasted_iota(jnp.int32, (DI, NHEADS), 0) // HEADDIM
        pick = (lane_head == lax.broadcasted_iota(jnp.int32, (DI, NHEADS), 1)).astype(f32)
        per_head = [
            total_of(sum_head, 0)[:, :NHEADS],
            total_of(sum_head, 1)[:, :NHEADS],
            mm_exact(skip_row, pick)[0:1, :],
        ]
        for k in range(3):
            for r in range(count):
                part_small[
                    r // 8, (r // 4) % 2, (r // 2) % 2, r % 2, :, pl.ds((3 + KCONV + k) * LANES, NHEADS)
                ] = per_head[k]

        for o in around:
            reduce_small.give(o)

    around = (3, 2, 1, 0)
    units = [(reduce_in, multiply_in, o) for o in around]
    units += [(reduce_out, multiply_out, o) for o in around]
    units += [(reduce_small, None, o) for o in around]
    totals = {}

    def advance(k, stage):
        if 0 <= k < len(units):
            reduce, multiply, o = units[k]
            if stage == 0 and multiply:
                multiply(o)
            if stage == 1:
                reduce.cores(o)
            if stage == 2:
                reduce.firsts(o)
            if stage == 3:
                totals[reduce] = reduce.seconds(o)

    for k in range(len(units) + 5):
        advance(k, 0)
        advance(k - 1, 1)
        advance(k - 3, 2)
        advance(k - 5, 3)
        if 3 <= k < 3 + length // Q:
            inputs_of(k - 3)
        if k == 3 + length // Q:
            small_parts()
    reduce_in.last(totals[reduce_in], inward)
    reduce_out.last(totals[reduce_out], outward)
    reduce_small.last(totals[reduce_small], small_out)

    def field(k, size):
        return small_out[:, pl.ds(k * LANES, size)]

    norm_grad[...] = field(0, width // count)
    for k in range(KCONV):
        kernel_grad[k : k + 1, :] = field(1 + k, DC // count)
    offset_grad[...] = field(1 + KCONV, DC // count)
    gain_grad[...] = field(2 + KCONV, DI // count)
    step_grad[...] = field(3 + KCONV, NHEADS)
    decay_grad[...] = field(4 + KCONV, NHEADS)
    skip_grad[...] = field(5 + KCONV, NHEADS)
    for reduce in (reduce_in, reduce_small, reduce_out):
        reduce.drain()


def finish_call(tokens, cotangent, norm_gain, grad_proj, gate_low, in_full, out_full, *sums):
    count = 32
    length, width = tokens.shape
    columns = grad_proj.shape[1]
    rows_in, rows_out = width // count, DI // count
    shape = jax.ShapeDtypeStruct
    space = pl.BlockSpec(memory_space=pltpu.VMEM)
    return pl.pallas_call(
        functools.partial(finish_kernel, rows_in, rows_out),
        name="finish",
        out_shape=(
            shape((length, width), bf16),
            shape((length, width), bf16),
            shape((rows_in, columns), f32),
            shape((rows_out, width), f32),
            shape((1, rows_in), f32),
            shape((KCONV, DC // count), f32),
            shape((1, DC // count), f32),
            shape((1, rows_out), f32),
            shape((1, NHEADS), f32),
            shape((1, NHEADS), f32),
            shape((1, NHEADS), f32),
        ),
        in_specs=[space] * 10,
        out_specs=[space] * 11,
        scratch_shapes=[
            pltpu.VMEM((length // Q, width, Q), bf16),
            pltpu.VMEM((1, FIELDS * LANES), f32),
            pltpu.VMEM((8, width), f32),
        ]
        + Reduce.scratch(rows_in, columns, columns // (2 * LANES) * LANES, bf16)
        + Reduce.scratch(rows_out, width, width // 2, bf16)
        + Reduce.scratch(1, FIELDS * LANES, FIELDS * LANES // 2, f32),
        compiler_params=pltpu.CompilerParams(
            collective_id=4, has_side_effects=True, vmem_limit_bytes=62 * 1024 * 1024
        ),
    )(tokens, cotangent, norm_gain, grad_proj, gate_low, in_full, out_full, *sums)


def rms_scale(values, weight):
    return values * lax.rsqrt(jnp.mean(values * values, axis=-1, keepdims=True) + epsilon) * weight


def local(
    dp_size,
    seq_size,
    tokens,
    cotangent,
    norm_gain,
    in_weight,
    conv_weight,
    conv_bias,
    dt_bias,
    a_log,
    d_skip,
    gate_gain,
    out_weight,
):
    axes = ("dp", "seq")
    sizes = [norm_gain.shape[0], conv_weight.size, conv_bias.shape[0], gate_gain.shape[0]]
    packed = jnp.concatenate([norm_gain, conv_weight.reshape(-1), conv_bias, gate_gain])
    quick = dp_size == 4 and seq_size == 8 and in_weight.shape[0] % 8 == 0
    quick = quick and out_weight.shape[0] % 8 == 0
    shards = (in_weight, out_weight, packed[None].astype(f32))
    if quick:
        in_full, out_full, packed = quick_gather_call(*shards)
    else:
        in_full, out_full, packed = gather_call({"dp": dp_size, "seq": seq_size}, *shards)
    in_full = in_full.reshape(-1, in_weight.shape[1])
    out_full = out_full.reshape(-1, out_weight.shape[1])
    packed = packed[:, 0]
    offsets = [0]
    for size in sizes:
        offsets.append(offsets[-1] + size)
    norm_full = packed[:, : offsets[1]].reshape(-1)
    taps_full = packed[:, offsets[1] : offsets[2]].reshape(-1, KCONV, conv_weight.shape[1])
    taps_full = jnp.swapaxes(taps_full, 0, 1).reshape(KCONV, DC)
    cbias_full = packed[:, offsets[2] : offsets[3]].reshape(1, DC)
    gain_full = packed[:, offsets[3] :].reshape(1, DI)
    heads = jnp.stack([dt_bias, a_log, d_skip])

    tokens = tokens[0]
    cotangent = cotangent[0]
    inputs = tokens.astype(f32)
    normed, norm_back = jax.vjp(rms_scale, inputs, norm_full)
    normed_low = normed.astype(bf16)
    proj = mm(normed_low, in_full).astype(bf16)
    grad_low = mm_nt(cotangent, out_full)
    gate_low, grad_proj, sum_conv, sum_gate, sum_head = ssd_call(
        seq_size, proj, grad_low, taps_full, cbias_full, heads, gain_full
    )
    sizes = {"dp": dp_size, "seq": seq_size}
    count = dp_size * seq_size
    if quick:
        results = finish_call(
            tokens,
            cotangent,
            norm_full[None],
            grad_proj,
            gate_low,
            in_full,
            out_full,
            sum_conv,
            sum_gate,
            sum_head,
        )
        block_out, input_grad, inward, outward = results[:4]
        norm_grad, kernel_grad, offset_grad, gain_grad, step_grad, decay_grad, skip_grad = results[4:]
        return (
            block_out[None],
            input_grad[None],
            norm_grad[0],
            inward,
            kernel_grad,
            offset_grad[0],
            step_grad[0],
            decay_grad[0],
            skip_grad[0],
            gain_grad[0],
            outward,
        )
    block_out = (inputs + mm(gate_low, out_full)).astype(bf16)
    outward = lax.dot_general(
        gate_low, cotangent, (((0,), (0,)), ((), ())), preferred_element_type=f32
    )
    inward = lax.dot_general(
        normed_low, grad_proj, (((0,), (0,)), ((), ())), preferred_element_type=f32
    )
    grad_normed = mm_nt(grad_proj, in_full)
    grad_inputs, norm_local = norm_back(grad_normed)
    input_grad = (grad_inputs + cotangent.astype(f32)).astype(bf16)

    conv_local = jnp.sum(sum_conv.reshape(KCONV + 1, 8, DC), axis=1)
    gate_local = jnp.sum(sum_gate.reshape(2, 8, DI), axis=1)
    head_local = jnp.sum(sum_head.reshape(2, 8, LANES), axis=1)[:, :NHEADS]
    skip_local = jnp.sum(gate_local[1].reshape(NHEADS, HEADDIM), axis=1)
    shared = jnp.concatenate([head_local.reshape(-1), skip_local])
    pieces = [
        norm_local.reshape(count, -1),
        jnp.swapaxes(conv_local[:KCONV].reshape(KCONV, count, -1), 0, 1).reshape(count, -1),
        conv_local[KCONV].reshape(count, -1),
        gate_local[0].reshape(count, -1),
        jnp.broadcast_to(shared[None], (count, shared.shape[0])),
    ]
    widths = [piece.shape[1] for piece in pieces]
    width = -(-sum(widths) // LANES) * LANES
    pieces.append(jnp.zeros((count, width - sum(widths)), f32))
    inward, outward, small = scatter_call(
        sizes,
        (4, 2, 1),
        inward.astype(bf16).reshape(count, -1, inward.shape[1]),
        outward.astype(bf16).reshape(count, -1, outward.shape[1]),
        jnp.concatenate(pieces, axis=1)[:, None],
    )
    at = [sum(widths[:k]) for k in range(6)]
    parts = [small[0, at[k] : at[k + 1]] for k in range(5)]
    norm_grad, kernel_grad, offset_grad, gain_grad, shared = parts
    kernel_grad = kernel_grad.reshape(KCONV, -1)
    step_grad, decay_grad, skip_grad = shared.reshape(3, NHEADS)
    return (
        block_out[None],
        input_grad[None],
        norm_grad,
        inward,
        kernel_grad,
        offset_grad,
        step_grad,
        decay_grad,
        skip_grad,
        gain_grad,
        outward,
    )


def solution(mesh):
    both = ("dp", "seq")
    return jax.shard_map(
        functools.partial(local, mesh.shape["dp"], mesh.shape["seq"]),
        mesh=mesh,
        in_specs=(
            P("dp", "seq", None),
            P("dp", "seq", None),
            P(both),
            P(both, None),
            P(None, both),
            P(both),
            P(),
            P(),
            P(),
            P(both),
            P(both, None),
        ),
        out_specs=(
            P("dp", "seq", None),
            P("dp", "seq", None),
            P(both),
            P(both, None),
            P(None, both),
            P(both),
            P(),
            P(),
            P(),
            P(both),
            P(both, None),
        ),
        check_vma=False,
    )
```
